32 devices in a mesh: dp: 8 (over y, x, core), seq: 4 (over z).
Axes of the slice: x: 2, y: 2, z: 4, core: 2. Of those that a mesh axis runs over, the one named last changes fastest.
Arguments:
- queries: bfloat16 [8, 1024, 2048], P('dp', 'seq'), may hold values from -6 to 6
- keys: bfloat16 [8, 1024, 1024], P('dp', 'seq'), may hold values from -6 to 6
- values: bfloat16 [8, 1024, 1024], P('dp', 'seq'), may hold values from -190 to 190
- segments: int32 [8, 1024], P('dp', 'seq'), may hold values from 0 to 2, never falling along the last dimension, each value on 1 to 640 neighbouring positions
- cotangent: bfloat16 [8, 1024, 2304], P('dp', 'seq'), may hold values from -6 to 6
- weight: float32 [2048, 2304], P(('dp', 'seq')), may hold values from -0.125 to 0.125
- first_moment: bfloat16 [2048, 2304], P(('dp', 'seq')), may hold values from -1 to 1
- first_scale: float32 [2048, 18], P(('dp', 'seq')), may hold values from 0.3 to 3
- second_moment: bfloat16 [2048, 2304], P(('dp', 'seq')), may hold values from 0.049804688 to 1
- second_scale: float32 [2048, 18], P(('dp', 'seq')), may hold values from 0.3 to 3
Outputs:
- layer_out: bfloat16 [8, 1024, 2304], P('dp', 'seq')
- new_weight: float32 [2048, 2304], P(('dp', 'seq'))
- new_first: bfloat16 [2048, 2304], P(('dp', 'seq'))
- new_first_scale: float32 [2048, 18], P(('dp', 'seq'))
- new_second: bfloat16 [2048, 2304], P(('dp', 'seq'))
- new_second_scale: float32 [2048, 18], P(('dp', 'seq'))
The draws below stay inside these ranges and needn't reach their ends.
Inputs may be any that keep to these rules, and one draw needn't show every extreme that they name: `segments`: document numbers never fall along a sequence; each sequence holds 3 documents, one of exactly 640 positions.
All inputs are finite; a program needn't handle non-finite values. Where the reference program divides by a largest or mean magnitude, that divisor is 1e-20 or more.
Results may differ from the reference program's by a relative error of at most 0.01.
Values may be sent and summed in bfloat16 or wider, within the bound.
A program may use at most 128 MiB of HBM per device.

```python
import math
import jax
import jax.numpy as jnp
import numpy as np
from jax import lax

HEADS = 16
KV_HEADS = 8
HEAD_DIM = 128
DO = 2304
GROUP = 128
DOCS = 3
QW = 2048
KW = 1024
LENGTH = 1024
SEQS = 8
DOC_MOST = 640


def draw_values(key, part):
    base_key, column_key, row_key = jax.random.split(jax.random.fold_in(key, 17), 3)
    columns = jnp.arange(KW, dtype=jnp.float32)
    column_multiplier = 10.0 ** (columns / (KW - 1)) * jax.random.uniform(column_key, (KW,), jnp.float32, 0.7, 1.4)
    row_factor = jnp.exp(jax.random.uniform(row_key, (SEQS, LENGTH, 1), jnp.float32, 0.0, math.log(10.0)))
    base = jnp.clip(jax.random.normal(base_key, (SEQS, LENGTH, KW), jnp.float32), -4.0, 4.0)
    return (base * column_multiplier * row_factor / 3.0).astype(jnp.bfloat16)


def level_of(stream_key, dims, shards, smallest, largest):
    def one(dim, shards_of):
        heights = jax.random.uniform(jax.random.fold_in(jax.random.fold_in(stream_key, 6), dim), (shards_of,), jnp.float32, smallest / len(shards), largest / len(shards))
        return jnp.repeat(jnp.exp(heights), dims[dim] // shards_of).reshape((-1,) + (1,) * (len(dims) - dim - 1))

    loudness = one(*shards[0])
    for cut in shards[1:]:
        loudness = loudness * one(*cut)
    return loudness


def length_profile(number_of, total, reach, slope):
    loads = [(1 << 20) // math.isqrt(rank ** slope) + 1 for rank in range(2, number_of + 1)]
    spare, holding = total - reach - (number_of - 1), [1] * (number_of - 1)
    while spare > 0:
        candidates = [i for i in range(number_of - 1) if holding[i] < reach]
        mass, budget = sum([loads[i] for i in candidates]), spare
        for i in candidates:
            addition = min(reach - holding[i], max(1, budget * loads[i] // mass), spare)
            holding[i] = holding[i] + addition
            spare = spare - addition
    return np.array([reach] + holding)


def uneven(own_key, number_of, total, most, lean):
    if number_of == 2:
        one = jax.random.randint(own_key, (), max(1, total - most), min(most, total - 1) + 1)
        return jnp.stack([one, total - one])
    sizes = jnp.asarray(length_profile(number_of, total, most, lean), jnp.int32)
    twos = (number_of - 1) // 2
    giver, sink = sizes[1:1 + 2 * twos:2], sizes[2:2 + 2 * twos:2]
    margin = jnp.minimum(giver - 1, most - sink)
    passed = jax.random.randint(jax.random.fold_in(own_key, 1), (twos,), 0, 1 << 20) % (margin + 1)
    sizes = sizes.at[1:1 + 2 * twos:2].set(giver - passed).at[2:2 + 2 * twos:2].set(sink + passed)
    return sizes[jax.random.permutation(jax.random.fold_in(own_key, 2), number_of)]


def bell_draw(stream_key, dims, width, limit, pieces=(), held_as=jnp.bfloat16):
    drawn = width * jax.random.normal(stream_key, dims, jnp.float32)
    if pieces:
        drawn = drawn * level_of(stream_key, dims, pieces, -0.22, 0.18)
    return jnp.clip(drawn, -limit, limit).astype(held_as)


def setup_inputs(seed: int = 0) -> dict:
    seeds = jax.random.split(jax.random.key(seed), 11)
    queries = bell_draw(seeds[0], (SEQS, LENGTH, QW), 1.0, 6.0, ((0, 8), (1, 4)))
    keys = bell_draw(seeds[1], (SEQS, LENGTH, KW), 1.0, 6.0, ((0, 8), (1, 4)))
    values = draw_values(jax.random.fold_in(seeds[10], 71), 0)
    segments = jax.vmap(lambda own: jnp.searchsorted(jnp.cumsum(uneven(own, DOCS, LENGTH, DOC_MOST, 0)), jnp.arange(LENGTH), side="right"))(jax.random.split(seeds[3], SEQS)).reshape((SEQS, LENGTH)).astype(jnp.int32)
    cotangent = bell_draw(seeds[4], (SEQS, LENGTH, DO), 1.0, 6.0, ((0, 8), (1, 4)))
    weight = bell_draw(seeds[5], (QW, DO), QW ** -0.5, 0.125, ((0, 32),), jnp.float32)
    first_moment = jnp.clip(jax.random.uniform(seeds[6], (QW, DO), jnp.float32, -1.0, 1.0) * level_of(seeds[6], (QW, DO), ((0, 32),), -0.4, 0.0), -1.0, 1.0).astype(jnp.bfloat16)
    first_scale = jnp.clip(jnp.exp(math.log(3.0) - 2.3025851 * jax.random.uniform(seeds[7], (QW, DO // GROUP), jnp.float32) ** level_of(seeds[7], (QW, DO // GROUP), ((0, 32),), -0.2, 0.2)), 0.3, 3.0)
    second_moment = jnp.clip(0.049804688 + 0.9501953 * jax.random.uniform(seeds[8], (QW, DO), jnp.float32) ** level_of(seeds[8], (QW, DO), ((0, 32),), -0.2, 0.2), 0.049804688, 1.0).astype(jnp.bfloat16)
    second_scale = jnp.clip(jnp.exp(math.log(3.0) - 2.3025851 * jax.random.uniform(seeds[9], (QW, DO // GROUP), jnp.float32) ** level_of(seeds[9], (QW, DO // GROUP), ((0, 32),), -0.2, 0.2)), 0.3, 3.0)
    return dict(queries=queries, keys=keys, values=values, segments=segments, cotangent=cotangent, weight=weight, first_moment=first_moment, first_scale=first_scale, second_moment=second_moment, second_scale=second_scale)


score_scale = 144.0 ** (-0.5)
soft_cap = 50.0
beta_first = 0.9
beta_second = 0.95
learn_rate = 0.001
decay_rate = 0.1

def quantize(blocks):
    grouped = blocks.astype(jnp.float32).reshape(blocks.shape[0], KV_HEADS, HEAD_DIM)
    scales = (lax.optimization_barrier(jnp.max(jnp.abs(grouped), axis=-1)) + 1e-06).astype(jnp.bfloat16)
    coded = (grouped / scales.astype(jnp.float32)[..., None]).astype(jnp.bfloat16)
    return (coded, scales)

def recover_values(coded, scales):
    return (coded.astype(jnp.float32) * scales.astype(jnp.float32)[..., None]).astype(jnp.bfloat16)

def attend(packed):
    query_seq, key_seq, value_seq, docs_seq = packed
    length = query_seq.shape[0]
    key_code, key_scale = quantize(key_seq)
    value_code, value_scale = quantize(value_seq)
    key_estimate = lax.optimization_barrier(recover_values(key_code, key_scale)).astype(jnp.float32)
    value_hat = lax.optimization_barrier(recover_values(value_code, value_scale)).astype(jnp.float32)
    grouped = query_seq.astype(jnp.float32).reshape(length, KV_HEADS, HEADS // KV_HEADS, HEAD_DIM)
    scores = jnp.einsum('qgrd,kgd->qgrk', grouped, key_estimate) * score_scale
    capped = soft_cap * jnp.tanh(scores / soft_cap)
    places = jnp.arange(length, dtype=jnp.int32)
    allowed = (docs_seq[:, None] == docs_seq[None, :]) & (places[None, :] <= places[:, None])
    weights = jnp.where(allowed[:, None, None, :], jnp.exp(capped), jnp.float32(0.0))
    totals = lax.optimization_barrier(jnp.sum(weights, axis=-1))
    rounded = lax.optimization_barrier(weights.astype(jnp.bfloat16)).astype(jnp.float32)
    mixed = jnp.einsum('qgrk,kgd->qgrd', rounded, value_hat)
    return (mixed / totals[..., None]).reshape(length, HEADS * HEAD_DIM).astype(jnp.bfloat16)

def decode(coded, scales):
    values_f = coded.astype(jnp.float32).reshape(coded.shape[0], -1, GROUP)
    return (scales[..., None] * jnp.sign(values_f) * jnp.sqrt(jnp.abs(values_f))).reshape(coded.shape)

def encode(moment):
    grouped = moment.reshape(moment.shape[0], -1, GROUP)
    scales = lax.optimization_barrier(jnp.max(jnp.abs(grouped), axis=-1)) + 1e-06
    coded = (grouped * jnp.abs(grouped) / (scales[..., None] * scales[..., None])).astype(jnp.bfloat16)
    return (coded.reshape(moment.shape), scales)

def reference(queries, keys, values, segments, cotangent, weight, first_moment, first_scale, second_moment, second_scale):
    attended = lax.map(attend, (queries, keys, values, segments))
    attended_flat = attended.reshape(-1, QW)
    weight_low = weight.astype(jnp.bfloat16)
    layer_out = jnp.dot(attended_flat, weight_low, preferred_element_type=jnp.float32).astype(jnp.bfloat16)
    layer_out = layer_out.reshape(SEQS, LENGTH, DO)
    gradient_matrix = jnp.dot(attended_flat.T, cotangent.reshape(-1, DO), preferred_element_type=jnp.float32)
    sum_squares = jnp.sum(gradient_matrix * gradient_matrix)
    rms_value = jnp.sqrt(sum_squares / (QW * DO) + 1e-06)
    clipped = gradient_matrix * jnp.minimum(jnp.float32(1.0), 1.0 / rms_value)
    first = beta_first * decode(first_moment, first_scale) + (1.0 - beta_first) * clipped
    second = beta_second * decode(second_moment, second_scale) + (1.0 - beta_second) * clipped * clipped
    new_weight = weight - learn_rate * (first / (jnp.sqrt(second) + 1e-08) + decay_rate * weight)
    new_first, new_first_scale = encode(first)
    new_second, new_second_scale = encode(second)
    return (layer_out, new_weight, new_first, new_first_scale, new_second, new_second_scale)
```

```python
import functools

import jax
import jax.numpy as jnp
from jax import lax
from jax.experimental import pallas as pl
from jax.experimental.pallas import tpu as pltpu
from jax.sharding import PartitionSpec as P

HEADS = 16
KV_HEADS = 8
HEAD_DIM = 128
GROUP = 128

score_scale = 144.0 ** (-0.5)
soft_cap = 50.0
beta_first = 0.9
beta_second = 0.95
learn_rate = 0.001
decay_rate = 0.1

MESH = pl.DeviceIdType.MESH


def longest(length):
    return length * 5 // 8


def reach_skips(tokens, n):
    skips = []
    for s in range(1, n):
        skip = max(0, s * tokens - longest(n * tokens)) // 128 * 128
        if skip < tokens:
            skips.append(skip)
    return tuple(skips)


def orders(bits):
    high = list(range(1, bits))
    return (high, high[::-1])


def flip(me, r):
    out = me
    b = 0
    while (1 << b) <= r:
        if r & (1 << b):
            digit = lax.rem(lax.div(me, 1 << b), 2)
            out = out + (1 - 2 * digit) * (1 << b)
        b += 1
    return out


def greet_bits(me, z, bits, n):
    barrier = pltpu.get_barrier_semaphore()
    for b in range(bits):
        pl.semaphore_signal(
            barrier, inc=1, device_id={"dp": flip(me, 1 << b), "seq": z}, device_id_type=MESH
        )
    for s in range(1, n):
        pl.semaphore_signal(
            barrier, inc=1, device_id={"dp": me, "seq": lax.rem(z + s, n)}, device_id_type=MESH
        )
    pl.semaphore_wait(barrier, bits + n - 1)


def main_kernel(
    bits, n, skips, ahead,
    q_ref, k_ref, v_ref, doc_ref, cot_ref, w_ref,
    out_ref, own_ref, sum_ref,
    kv_all, doc_all, w_all, att, own_doc, acc, tot,
    sb, rb, zs, zr, grad, tot_s, tot_r,
    ws, wr, ks, kr, ds_, dr, ts, tr, bs, br, zss, zsr, qs, qr,
):
    me = lax.axis_index("dp")
    z = lax.axis_index("seq")
    tokens = k_ref.shape[0]
    rows, width = w_ref.shape
    half = width // 2
    big = n * rows
    count = 1 << bits
    per = count // KV_HEADS
    steps = len(skips)
    right, left = lax.rem(z + 1, n), lax.rem(z + n - 1, n)
    group_me = lax.div(me, per)
    sends = []

    def descriptor(src, dst, ssem, rsem, dp, seq):
        return pltpu.make_async_remote_copy(
            src_ref=src, dst_ref=dst, send_sem=ssem, recv_sem=rsem,
            device_id={"dp": dp, "seq": seq}, device_id_type=MESH,
        )

    def go(make, cond=None):
        if cond is None:
            make().start()
        else:

            @pl.when(cond)
            def _():
                make().start()

        sends.append((make, cond))

    def when(cond, act):
        if cond is None:
            act()
        else:
            pl.when(cond)(act)

    own_rows = pl.ds(pl.multiple_of(z * tokens, 128), tokens)

    def restore_group(g, _):
        cols = pl.ds(pl.multiple_of(g * HEAD_DIM, 128), HEAD_DIM)
        for part, ref in enumerate((k_ref, v_ref)):
            x = ref[:, cols].astype(jnp.float32)
            scale = jnp.max(jnp.abs(x), axis=-1, keepdims=True) + 1e-06
            wide = scale.astype(jnp.bfloat16).astype(jnp.float32)
            coded = (x / wide).astype(jnp.bfloat16).astype(jnp.float32)
            kv_all[g, part, own_rows, :] = (coded * wide).astype(jnp.bfloat16)
        return 0

    lax.fori_loop(0, KV_HEADS, restore_group, 0)
    doc_all[:, own_rows] = doc_ref[...]
    own_doc[...] = jnp.broadcast_to(doc_ref[0:1, :], (128, tokens)).T

    def w_rows(block, zz):
        return pl.ds(pl.multiple_of((block * n + zz) * rows, 16), rows)

    w_all[w_rows(me, z), :] = w_ref[...].astype(jnp.bfloat16)
    for s in range(1, steps + 1):
        if skips[s - 1]:

            @pl.when(z >= s)
            def _(s=s):
                stale = pl.ds(pl.multiple_of((z - s) * tokens, 128), skips[s - 1])
                for g in range(KV_HEADS):
                    for part in range(2):
                        kv_all[g, part, stale, :] = jnp.zeros(
                            (skips[s - 1], HEAD_DIM), jnp.bfloat16
                        )

    greet_bits(me, z, bits, n)

    def room(direction, s):
        if direction == 0:
            return (z >= s - 1) & (z < n - 1)
        return (z <= n - s) & (z > 0)

    def landed(direction, s):
        return z >= s if direction == 0 else z <= n - 1 - s

    def group_of(i):
        return flip(group_me, KV_HEADS - 1 - i)

    def kv_copy(s, i, at):
        skip = skips[s - 1]
        start = pl.multiple_of(at * tokens + skip, 128)
        part = kv_all.at[group_of(i), :, pl.ds(start, tokens - skip), :]
        return descriptor(part, part, ks.at[s - 1, i], kr.at[s - 1, i], me, right)

    def kv_send(s, i, cond):
        go(lambda: kv_copy(s, i, z - (s - 1)), cond)

    def kv_relay(i):
        for s in range(1, steps + 1):

            @pl.when(landed(0, s))
            def _(s=s):
                kv_copy(s, i, z - s).wait_recv()

            if s < steps:
                kv_send(s + 1, i, room(0, s + 1))

    def w_hop(direction, s, at):
        part = w_all.at[w_rows(me, at), :]
        return descriptor(
            part, part, ws.at[direction, s - 1], wr.at[direction, s - 1],
            me, right if direction == 0 else left,
        )

    def w_send(direction, s):
        at = z - (s - 1) if direction == 0 else z + (s - 1)
        go(lambda: w_hop(direction, s, at), room(direction, s))

    w_tree = [list(order) + [0] for order in orders(bits)]
    w_stage = []
    for h in range(2):
        seen, levels = [0], []
        for b in w_tree[h]:
            fresh = [r | (1 << b) for r in seen]
            levels.append(fresh)
            seen = seen + fresh
        w_stage.append(levels)

    def w_copy(zz, h, r, to):
        part = w_all.at[w_rows(flip(me, r), zz), pl.ds(h * half, half)]
        return part, to

    def w_forward(zz, h, r, cond):
        order = w_tree[h]
        last = -1
        for i, b in enumerate(order):
            if r & (1 << b):
                last = i
        for b in order[last + 1:]:
            nr = r | (1 << b)

            def make(b=b, nr=nr):
                part = w_all.at[w_rows(flip(me, r), zz), pl.ds(h * half, half)]
                return descriptor(
                    part, part, ts.at[zz, h, nr], tr.at[zz, h, nr], flip(me, 1 << b), z
                )

            go(make, cond)

    def w_wait(zz, h, r, cond):
        def act():
            part = w_all.at[w_rows(flip(me, r), zz), pl.ds(h * half, half)]
            descriptor(part, part, ts.at[zz, h, r], tr.at[zz, h, r], me, right).wait_recv()

        when(cond, act)

    def w_level(zz, level, cond):
        for j in range(len(w_stage[0][level])):
            for h in range(2):
                r = w_stage[h][level][j]
                w_wait(zz, h, r, cond)
                if level < bits - 1:
                    w_forward(zz, h, r, cond)

    def w_arrive(direction, s):
        zz = z - s if direction == 0 else z + s

        @pl.when(landed(direction, s))
        def _():
            w_hop(direction, s, zz).wait_recv()

        if s < n - 1:
            w_send(direction, s + 1)
        for h in range(2):
            w_forward(zz, h, 0, landed(direction, s))

    last_step = KV_HEADS
    events = {i: [] for i in range(last_step + 1)}

    def plan(i, act):
        events[min(i, last_step)].append(act)

    for level in range(bits - 1):
        plan(level, lambda level=level: w_level(z, level, None))
    for s in range(1, n):
        at = 2 * (s - 1) * 3 // (n - 1)
        for direction in range(2):
            zz = z - s if direction == 0 else z + s
            plan(at, lambda d=direction, s=s: w_arrive(d, s))
            for level in range(bits - 1):
                plan(
                    at + 1 + level,
                    lambda zz=zz, level=level, d=direction, s=s: w_level(
                        zz, level, landed(d, s)
                    ),
                )

    for direction in range(2):
        w_send(direction, 1)
    for h in range(2):
        w_forward(z, h, 0, None)
    doc_copies = []
    for s in range(1, n):
        def make(s=s):
            slot = doc_all.at[:, own_rows]
            return descriptor(
                slot, slot, ds_.at[s - 1], dr.at[s - 1], me, lax.rem(z + s, n)
            )

        go(make)
        doc_copies.append(make)
    for i in range(KV_HEADS):
        kv_send(1, i, (z < n - 1) if i < ahead else ((z == 0) if n > 1 else None))

    query_at = lax.broadcasted_iota(jnp.int32, (tokens, tokens), 0)
    key_at = lax.broadcasted_iota(jnp.int32, (tokens, tokens), 1)
    lo = jnp.maximum(z - steps, 0)
    pair = HEADS // KV_HEADS

    def attend_group(i):
        g = group_of(i)
        acc[...] = jnp.zeros_like(acc)
        tot[...] = jnp.zeros_like(tot)

        def block(j, _):
            at = pl.ds(pl.multiple_of(j * tokens, 128), tokens)
            same = own_doc[:, 0:1] == doc_all[0:1, at]
            allowed = same & (key_at + (j - z) * tokens <= query_at)
            key = kv_all[g, 0, at, :]
            value = kv_all[g, 1, at, :]
            for hd in range(pair):
                cols = pl.ds(pl.multiple_of((g * pair + hd) * HEAD_DIM, 128), HEAD_DIM)
                scores = lax.dot_general(
                    q_ref[:, cols], key, (((1,), (1,)), ((), ())),
                    preferred_element_type=jnp.float32,
                )
                capped = soft_cap * jnp.tanh(scores * (score_scale / soft_cap))
                weights = jnp.where(allowed, jnp.exp(capped), 0.0)
                tot[hd] = tot[hd] + jnp.sum(weights, axis=-1, keepdims=True)
                acc[hd] = acc[hd] + jnp.dot(
                    weights.astype(jnp.bfloat16), value, preferred_element_type=jnp.float32
                )
            return 0

        lax.fori_loop(lo, z + 1, block, 0)
        for hd in range(pair):
            cols = pl.ds(pl.multiple_of((g * pair + hd) * HEAD_DIM, 128), HEAD_DIM)
            att[:, cols] = (acc[hd] / tot[hd]).astype(att.dtype)

    tree = [[0] + list(order) for order in orders(bits)]

    def first_bit(r, h):
        for b in tree[h]:
            if r & (1 << b):
                return b

    def sources(r, h):
        out = []
        for b in tree[h]:
            if r & (1 << b):
                break
            out.append(r | (1 << b))
        return out

    def block_t(r):
        start = pl.multiple_of(flip(me, r) * big, 128)
        return att[:, pl.ds(start, big)].T

    def reduce_block(r, h, block):
        value = jnp.dot(
            block, cot_ref[:, h * half:(h + 1) * half], preferred_element_type=jnp.float32
        )
        for src in sources(r, h):
            descriptor(
                sb.at[h, src], rb.at[h, src], bs.at[h, src], br.at[h, src], me, right
            ).wait_recv()
            value = value + rb[h, src].astype(jnp.float32)
        if r == 0:
            grad[:, h * half:(h + 1) * half] = value
            return
        sb[h, r] = value.astype(jnp.bfloat16)
        b = first_bit(r, h)
        go(lambda: descriptor(
            sb.at[h, r], rb.at[h, r], bs.at[h, r], br.at[h, r], flip(me, 1 << b), z
        ))

    late = []
    for i in range(KV_HEADS):
        kv_relay(i)
        if i + ahead < KV_HEADS:
            kv_send_next = i + ahead
            go(
                lambda j=kv_send_next: kv_copy(1, j, z), (z > 0) & (z < n - 1)
            )
        for act in events[i]:
            act()
        if i == 0:
            for make in doc_copies:
                make().wait_recv()
        attend_group(i)
        for r in range((KV_HEADS - i) * per - 1, (KV_HEADS - 1 - i) * per - 1, -1):
            if r == 0:
                continue
            block = block_t(r)
            for h in range(2):
                if len(sources(r, h)) > 1:
                    late.append((r, h))
                else:
                    reduce_block(r, h, block)
        if i == KV_HEADS - 2:
            for r, h in late:
                reduce_block(r, h, block_t(r))
            late = []
    for r, h in late:
        reduce_block(r, h, block_t(r))

    for act in events[last_step]:
        act()
    every = [(z, None)]
    for s in range(1, n):
        for direction in range(2):
            zz = z - s if direction == 0 else z + s
            every.append((zz, landed(direction, s)))
    for zz, cond in every:
        w_level(zz, bits - 1, cond)

    def project(c, _):
        cols = pl.ds(pl.multiple_of(c * 256, 256), 256)
        out_ref[:, cols] = jnp.dot(
            att[...], w_all[:, cols], preferred_element_type=jnp.float32
        ).astype(out_ref.dtype)
        return 0

    lax.fori_loop(0, width // 256, project, 0)

    last_block = block_t(0)
    for h in range(2):
        reduce_block(0, h, last_block)

    def part(zz, h):
        start = pl.multiple_of(zz * rows, 16)
        return grad[pl.ds(start, rows), h * half:(h + 1) * half]

    ring = {}
    for s in range(n):
        for h in range(2):
            shift = (2 * n - 1 - s) if h == 0 else (1 + s)
            at = lax.rem(z + shift, n)
            value = part(at, h)
            if s:
                ring[h, s - 1]().wait_recv()
                value = value + zr[h, s - 1].astype(jnp.float32)
            if s < n - 1:
                zs[h, s] = value.astype(jnp.bfloat16)

                def make(h=h, s=s):
                    return descriptor(
                        zs.at[h, s], zr.at[h, s], zss.at[h, s], zsr.at[h, s],
                        me, right if h == 0 else left,
                    )

                go(make)
                ring[h, s] = make
            else:
                own_ref[:, h * half:(h + 1) * half] = value

    own = own_ref[...]
    total = jnp.broadcast_to(
        jnp.sum(jnp.sum(own * own, axis=1, keepdims=True), axis=0, keepdims=True), (8, 128)
    )
    for b in range(bits):
        tot_s[b] = total

        def make(b=b):
            return descriptor(
                tot_s.at[b], tot_r.at[b], qs.at[b], qr.at[b], flip(me, 1 << b), z
            )

        go(make)
        make().wait_recv()
        total = total + tot_r[b]
    tot_s[bits] = total
    last = []
    for s in range(1, n):
        def make(s=s):
            i = bits + s - 1
            return descriptor(
                tot_s.at[bits], tot_r.at[i], qs.at[i], qr.at[i], me, lax.rem(z + s, n)
            )

        go(make)
        last.append(make)
    for s in range(1, n):
        last[s - 1]().wait_recv()
        total = total + tot_r[bits + s - 1]
    sum_ref[...] = total
    for make, cond in sends:
        when(cond, lambda make=make: make().wait_send())


def main_step(q, k, v, docs, cot, w, bits, n):
    tokens = k.shape[0]
    rows, width = w.shape
    half = width // 2
    count = 1 << bits
    skips = reach_skips(tokens, n)
    steps = len(skips)
    sem = pltpu.SemaphoreType.DMA
    vm = pl.BlockSpec(memory_space=pltpu.VMEM)
    pair = HEADS // KV_HEADS
    bf16, f32 = jnp.bfloat16, jnp.float32
    return pl.pallas_call(
        functools.partial(main_kernel, bits, n, skips, 2),
        out_shape=(
            jax.ShapeDtypeStruct((tokens, width), bf16),
            jax.ShapeDtypeStruct((rows, width), f32),
            jax.ShapeDtypeStruct((8, 128), f32),
        ),
        in_specs=[vm] * 6,
        out_specs=(vm,) * 3,
        scratch_shapes=[
            pltpu.VMEM((KV_HEADS, 2, n * tokens, HEAD_DIM), bf16),
            pltpu.VMEM((8, n * tokens), jnp.int32),
            pltpu.VMEM((count * n * rows, width), bf16),
            pltpu.VMEM((tokens, HEADS * HEAD_DIM), bf16),
            pltpu.VMEM((tokens, 128), jnp.int32),
            pltpu.VMEM((pair, tokens, HEAD_DIM), f32),
            pltpu.VMEM((pair, tokens, 1), f32),
            pltpu.VMEM((2, count, n * rows, half), bf16),
            pltpu.VMEM((2, count, n * rows, half), bf16),
            pltpu.VMEM((2, n - 1, rows, half), bf16),
            pltpu.VMEM((2, n - 1, rows, half), bf16),
            pltpu.VMEM((n * rows, width), f32),
            pltpu.VMEM((bits + 1, 8, 128), f32),
            pltpu.VMEM((bits + n - 1, 8, 128), f32),
            sem((2, n - 1)), sem((2, n - 1)),
            sem((steps, KV_HEADS)), sem((steps, KV_HEADS)),
            sem((n - 1,)), sem((n - 1,)),
            sem((n, 2, count)), sem((n, 2, count)),
            sem((2, count)), sem((2, count)),
            sem((2, n - 1)), sem((2, n - 1)),
            sem((bits + n - 1,)), sem((bits + n - 1,)),
        ],
        compiler_params=pltpu.CompilerParams(
            collective_id=0, has_side_effects=True, vmem_limit_bytes=62 * 1024 * 1024
        ),
    )(q, k, v, docs, cot, w)


def adam_kernel(
    entries,
    grad_ref, sum_ref, w_ref, m1_ref, s1_ref, m2_ref, s2_ref,
    nw_ref, n1_ref, ns1_ref, n2_ref, ns2_ref,
):
    width = w_ref.shape[1]
    rms = jnp.sqrt(sum_ref[0:1, :] / entries + 1e-06)
    factor = jnp.minimum(1.0, 1.0 / rms)

    def decode(coded, scale):
        x = coded.astype(jnp.float32)
        root = scale * jnp.sqrt(jnp.abs(x))
        return jnp.where(x < 0, -root, root)

    def encode(x):
        scale = jnp.max(jnp.abs(x), axis=-1, keepdims=True) + 1e-06
        return (x * jnp.abs(x) / (scale * scale)).astype(jnp.bfloat16), scale

    for g in range(width // GROUP):
        cols = slice(g * GROUP, (g + 1) * GROUP)
        clipped = grad_ref[:, cols] * factor
        first = beta_first * decode(m1_ref[:, cols], s1_ref[:, g:g + 1]) + (
            1.0 - beta_first
        ) * clipped
        second = (
            beta_second * decode(m2_ref[:, cols], s2_ref[:, g:g + 1])
            + (1.0 - beta_second) * clipped * clipped
        )
        weight = w_ref[:, cols]
        nw_ref[:, cols] = weight - learn_rate * (
            first / (jnp.sqrt(second) + 1e-08) + decay_rate * weight
        )
        n1_ref[:, cols], ns1_ref[:, g:g + 1] = encode(first)
        n2_ref[:, cols], ns2_ref[:, g:g + 1] = encode(second)


def adam(grad, total, weight, m1, s1, m2, s2, entries):
    vm = pl.BlockSpec(memory_space=pltpu.VMEM)
    like = lambda a: jax.ShapeDtypeStruct(a.shape, a.dtype)
    return pl.pallas_call(
        functools.partial(adam_kernel, entries),
        out_shape=(like(weight), like(m1), like(s1), like(m2), like(s2)),
        in_specs=[vm] * 7,
        out_specs=(vm,) * 5,
    )(grad, total, weight, m1, s1, m2, s2)


def local(
    bits, n,
    queries, keys, values, segments, cotangent, weight,
    first_moment, first_scale, second_moment, second_scale,
):
    docs = segments[0]
    tokens = docs.shape[0]
    rows, width = weight.shape
    layer_out, grad, total = main_step(
        queries[0], keys[0], values[0],
        jnp.broadcast_to(docs[None, :], (8, tokens)),
        cotangent[0], weight, bits, n,
    )
    entries = float((1 << bits) * n * rows * width)
    updated = adam(
        grad, total, weight, first_moment, first_scale, second_moment, second_scale, entries
    )
    return (layer_out[None], *updated)


def solution(mesh):
    bits = mesh.shape["dp"].bit_length() - 1
    n = mesh.shape["seq"]
    shard = P(("dp", "seq"), None)
    tok = P("dp", "seq", None)
    return jax.shard_map(
        functools.partial(local, bits, n),
        mesh=mesh,
        in_specs=(tok, tok, tok, P("dp", "seq"), tok, shard, shard, shard, shard, shard),
        out_specs=(tok, shard, shard, shard, shard, shard),
        check_vma=False,
    )
```

```python
import functools

import jax
import jax.numpy as jnp
from jax import lax
from jax.experimental import pallas as pl
from jax.experimental.pallas import tpu as pltpu
from jax.sharding import PartitionSpec as P

HEADS = 16
KV_HEADS = 8
HEAD_DIM = 128
GROUP = 128

score_scale = 144.0 ** (-0.5)
soft_cap = 50.0
beta_first = 0.9
beta_second = 0.95
learn_rate = 0.001
decay_rate = 0.1

MESH = pl.DeviceIdType.MESH


def longest(length):
    return length * 5 // 8


def reach_skips(tokens, n):
    skips = []
    for s in range(1, n):
        skip = max(0, s * tokens - longest(n * tokens)) // 128 * 128
        if skip < tokens:
            skips.append(skip)
    return tuple(skips)


def orders(bits):
    high = list(range(1, bits))
    return (high, high[::-1])


def flip(me, r):
    out = me
    b = 0
    while (1 << b) <= r:
        if r & (1 << b):
            digit = lax.rem(lax.div(me, 1 << b), 2)
            out = out + (1 - 2 * digit) * (1 << b)
        b += 1
    return out


def greet_bits(me, z, bits, n):
    barrier = pltpu.get_barrier_semaphore()
    for b in range(bits):
        pl.semaphore_signal(
            barrier, inc=1, device_id={"dp": flip(me, 1 << b), "seq": z}, device_id_type=MESH
        )
    for s in range(1, n):
        pl.semaphore_signal(
            barrier, inc=1, device_id={"dp": me, "seq": lax.rem(z + s, n)}, device_id_type=MESH
        )
    pl.semaphore_wait(barrier, bits + n - 1)


def main_kernel(
    bits, n, skips, ahead,
    q_ref, k_ref, v_ref, doc_ref, cot_ref, w_ref,
    out_ref, own_ref, sum_ref,
    kv_all, doc_all, w_all, att, own_doc, acc, tot,
    sb, rb, zs, zr, grad, tot_s, tot_r,
    ws, wr, ks, kr, ds_, dr, ts, tr, bs, br, zss, zsr, qs, qr,
):
    me = lax.axis_index("dp")
    z = lax.axis_index("seq")
    tokens = k_ref.shape[0]
    rows, width = w_ref.shape
    half = width // 2
    big = n * rows
    count = 1 << bits
    per = count // KV_HEADS
    steps = len(skips)
    right, left = lax.rem(z + 1, n), lax.rem(z + n - 1, n)
    group_me = lax.div(me, per)
    sends = []

    def descriptor(src, dst, ssem, rsem, dp, seq):
        return pltpu.make_async_remote_copy(
            src_ref=src, dst_ref=dst, send_sem=ssem, recv_sem=rsem,
            device_id={"dp": dp, "seq": seq}, device_id_type=MESH,
        )

    def go(make, cond=None):
        if cond is None:
            make().start()
        else:

            @pl.when(cond)
            def _():
                make().start()

        sends.append((make, cond))

    def when(cond, act):
        if cond is None:
            act()
        else:
            pl.when(cond)(act)

    own_rows = pl.ds(pl.multiple_of(z * tokens, 128), tokens)

    def restore_group(g, _):
        cols = pl.ds(pl.multiple_of(g * HEAD_DIM, 128), HEAD_DIM)
        for part, ref in enumerate((k_ref, v_ref)):
            x = ref[:, cols].astype(jnp.float32)
            scale = jnp.max(jnp.abs(x), axis=-1, keepdims=True) + 1e-06
            wide = scale.astype(jnp.bfloat16).astype(jnp.float32)
            coded = (x / wide).astype(jnp.bfloat16).astype(jnp.float32)
            kv_all[g, part, own_rows, :] = (coded * wide).astype(jnp.bfloat16)
        return 0

    lax.fori_loop(0, KV_HEADS, restore_group, 0)
    doc_all[:, own_rows] = jnp.broadcast_to(doc_ref[...], (8, tokens))
    own_doc[...] = jnp.broadcast_to(doc_ref[0:1, :], (128, tokens)).T

    def w_rows(block, zz):
        return pl.ds(pl.multiple_of((block * n + zz) * rows, 16), rows)

    w_all[w_rows(me, z), :] = w_ref[...].astype(jnp.bfloat16)
    for s in range(1, steps + 1):
        if skips[s - 1]:

            @pl.when(z >= s)
            def _(s=s):
                stale = pl.ds(pl.multiple_of((z - s) * tokens, 128), skips[s - 1])
                for g in range(KV_HEADS):
                    for part in range(2):
                        kv_all[g, part, stale, :] = jnp.zeros(
                            (skips[s - 1], HEAD_DIM), jnp.bfloat16
                        )

    greet_bits(me, z, bits, n)

    def room(direction, s):
        if direction == 0:
            return (z >= s - 1) & (z < n - 1)
        return (z <= n - s) & (z > 0)

    def landed(direction, s):
        return z >= s if direction == 0 else z <= n - 1 - s

    def group_of(i):
        return flip(group_me, KV_HEADS - 1 - i)

    def kv_copy(s, i, at):
        skip = skips[s - 1]
        start = pl.multiple_of(at * tokens + skip, 128)
        part = kv_all.at[group_of(i), :, pl.ds(start, tokens - skip), :]
        return descriptor(part, part, ks.at[s - 1, i], kr.at[s - 1, i], me, right)

    def kv_send(s, i, cond):
        go(lambda: kv_copy(s, i, z - (s - 1)), cond)

    def kv_relay(i):
        for s in range(1, steps + 1):

            @pl.when(landed(0, s))
            def _(s=s):
                kv_copy(s, i, z - s).wait_recv()

            if s < steps:
                kv_send(s + 1, i, room(0, s + 1))

    def w_hop(direction, s, at):
        part = w_all.at[w_rows(me, at), :]
        return descriptor(
            part, part, ws.at[direction, s - 1], wr.at[direction, s - 1],
            me, right if direction == 0 else left,
        )

    def w_send(direction, s):
        at = z - (s - 1) if direction == 0 else z + (s - 1)
        go(lambda: w_hop(direction, s, at), room(direction, s))

    w_tree = [list(order) + [0] for order in orders(bits)]
    w_stage = []
    for h in range(2):
        seen, levels = [0], []
        for b in w_tree[h]:
            fresh = [r | (1 << b) for r in seen]
            levels.append(fresh)
            seen = seen + fresh
        w_stage.append(levels)

    def w_forward(zz, h, r, cond):
        order = w_tree[h]
        last = -1
        for i, b in enumerate(order):
            if r & (1 << b):
                last = i
        for b in order[last + 1:]:
            nr = r | (1 << b)

            def make(b=b, nr=nr):
                part = w_all.at[w_rows(flip(me, r), zz), pl.ds(h * half, half)]
                return descriptor(
                    part, part, ts.at[zz, h, nr], tr.at[zz, h, nr], flip(me, 1 << b), z
                )

            go(make, cond)

    def w_wait(zz, h, r, cond):
        def act():
            part = w_all.at[w_rows(flip(me, r), zz), pl.ds(h * half, half)]
            descriptor(part, part, ts.at[zz, h, r], tr.at[zz, h, r], me, right).wait_recv()

        when(cond, act)

    def w_level(zz, level, cond):
        for j in range(len(w_stage[0][level])):
            for h in range(2):
                r = w_stage[h][level][j]
                w_wait(zz, h, r, cond)
                if level < bits - 1:
                    w_forward(zz, h, r, cond)

    def source(direction, s):
        return z - s if direction == 0 else z + s

    def w_arrive(direction, s):
        zz = source(direction, s)

        @pl.when(landed(direction, s))
        def _():
            w_hop(direction, s, zz).wait_recv()

        for h in range(2):
            w_forward(zz, h, 0, landed(direction, s))

    def arrive(s):
        for direction in range(2):
            w_arrive(direction, s)

    def level(s, k):
        if s == 0:
            w_level(z, k, None)
        else:
            for direction in range(2):
                w_level(source(direction, s), k, landed(direction, s))

    last_step = KV_HEADS
    events = {i: [] for i in range(last_step)}

    def plan(i, act):
        events[min(i, last_step - 1)].append(act)

    plan(3, lambda: w_send(0, 1))
    for k in range(bits - 1):
        plan(2 + 2 * k, lambda k=k: level(0, k))
    if n > 1:
        plan(6, lambda: arrive(1))

    w_send(1, 1)
    doc_copies = []
    for s in range(1, n):
        def make(s=s):
            slot = doc_all.at[:, own_rows]
            return descriptor(
                slot, slot, ds_.at[s - 1], dr.at[s - 1], me, lax.rem(z + s, n)
            )

        go(make)
        doc_copies.append(make)
    for i in range(KV_HEADS):
        kv_send(1, i, (z < n - 1) if i < ahead else (z == 0))
    for h in range(2):
        w_forward(z, h, 0, None)

    query_at = lax.broadcasted_iota(jnp.int32, (tokens, tokens), 0)
    key_at = lax.broadcasted_iota(jnp.int32, (tokens, tokens), 1)
    lo = jnp.maximum(z - steps, 0)
    pair = HEADS // KV_HEADS

    def attend_group(i):
        g = group_of(i)
        acc[...] = jnp.zeros_like(acc)
        tot[...] = jnp.zeros_like(tot)

        def block(j, _):
            at = pl.ds(pl.multiple_of(j * tokens, 128), tokens)
            same = own_doc[:, 0:1] == doc_all[0:1, at]
            allowed = same & (key_at + (j - z) * tokens <= query_at)
            key = kv_all[g, 0, at, :]
            value = kv_all[g, 1, at, :]
            for hd in range(pair):
                cols = pl.ds(pl.multiple_of((g * pair + hd) * HEAD_DIM, 128), HEAD_DIM)
                scores = lax.dot_general(
                    q_ref[:, cols], key, (((1,), (1,)), ((), ())),
                    preferred_element_type=jnp.float32,
                )
                capped = soft_cap * jnp.tanh(scores * (score_scale / soft_cap))
                weights = jnp.where(allowed, jnp.exp(capped), 0.0)
                tot[hd] = tot[hd] + jnp.sum(weights, axis=-1, keepdims=True)
                acc[hd] = acc[hd] + jnp.dot(
                    weights.astype(jnp.bfloat16), value, preferred_element_type=jnp.float32
                )
            return 0

        lax.fori_loop(lo, z + 1, block, 0)
        for hd in range(pair):
            cols = pl.ds(pl.multiple_of((g * pair + hd) * HEAD_DIM, 128), HEAD_DIM)
            att[:, cols] = (acc[hd] / tot[hd]).astype(att.dtype)

    tree = [[0] + list(order) for order in orders(bits)]

    def first_bit(r, h):
        for b in tree[h]:
            if r & (1 << b):
                return b

    def sources(r, h):
        out = []
        for b in tree[h]:
            if r & (1 << b):
                break
            out.append(r | (1 << b))
        return out

    def block_t(r):
        start = pl.multiple_of(flip(me, r) * big, 128)
        return att[:, pl.ds(start, big)].T

    def reduce_block(r, h, block):
        value = jnp.dot(
            block, cot_ref[:, h * half:(h + 1) * half], preferred_element_type=jnp.float32
        )
        for src in sources(r, h):
            descriptor(
                sb.at[h, src], rb.at[h, src], bs.at[h, src], br.at[h, src], me, right
            ).wait_recv()
            value = value + rb[h, src].astype(jnp.float32)
        if r == 0:
            grad[:, h * half:(h + 1) * half] = value
            return
        sb[h, r] = value.astype(jnp.bfloat16)
        b = first_bit(r, h)
        go(lambda: descriptor(
            sb.at[h, r], rb.at[h, r], bs.at[h, r], br.at[h, r], flip(me, 1 << b), z
        ))

    late = []
    for i in range(KV_HEADS):
        kv_relay(i)
        if i + ahead < KV_HEADS:
            kv_send_next = i + ahead
            go(
                lambda j=kv_send_next: kv_copy(1, j, z), (z > 0) & (z < n - 1)
            )
        for act in events[i]:
            act()
        if i == 0:
            for make in doc_copies:
                make().wait_recv()
        attend_group(i)
        for r, h in late:
            reduce_block(r, h, block_t(r))
        late = []
        for r in range((KV_HEADS - i) * per - 1, (KV_HEADS - 1 - i) * per - 1, -1):
            if r == 0:
                continue
            block = block_t(r)
            for h in range(2):
                if len(sources(r, h)) > 1 and i < 4:
                    late.append((r, h))
                else:
                    reduce_block(r, h, block)

    def part(zz, h):
        start = pl.multiple_of(zz * rows, 16)
        return grad[pl.ds(start, rows), h * half:(h + 1) * half]

    ring = {}

    def ring_step(s):
        for h in range(2):
            shift = (2 * n - 1 - s) if h == 0 else (1 + s)
            at = lax.rem(z + shift, n)
            value = part(at, h)
            if s:
                ring[h, s - 1]().wait_recv()
                value = value + zr[h, s - 1].astype(jnp.float32)
            if s < n - 1:
                zs[h, s] = value.astype(jnp.bfloat16)

                def make(h=h, s=s):
                    return descriptor(
                        zs.at[h, s], zr.at[h, s], zss.at[h, s], zsr.at[h, s],
                        me, right if h == 0 else left,
                    )

                go(make)
                ring[h, s] = make
            else:
                own_ref[:, h * half:(h + 1) * half] = value

    def relay_w(s):
        for direction in range(2):
            w_send(direction, s)

    if n > 2:
        relay_w(2)
        arrive(2)
    if n > 3:
        relay_w(3)
    last_block = block_t(0)
    for h in range(2):
        reduce_block(0, h, last_block)
    for s in range(n):
        ring_step(s)
        if s + 3 < n:
            arrive(s + 3)
            if s + 4 < n:
                relay_w(s + 4)
        if 0 < s < n - 1:
            for k in range(min(s, bits - 1)):
                level(s - k, k)

    own = own_ref[...]
    total = jnp.broadcast_to(
        jnp.sum(jnp.sum(own * own, axis=1, keepdims=True), axis=0, keepdims=True), (8, 128)
    )
    for b in range(bits):
        tot_s[b] = total

        def make(b=b):
            return descriptor(
                tot_s.at[b], tot_r.at[b], qs.at[b], qr.at[b], flip(me, 1 << b), z
            )

        go(make)
        make().wait_recv()
        total = total + tot_r[b]
    tot_s[bits] = total
    last = []
    for s in range(1, n):
        def make(s=s):
            i = bits + s - 1
            return descriptor(
                tot_s.at[bits], tot_r.at[i], qs.at[i], qr.at[i], me, lax.rem(z + s, n)
            )

        go(make)
        last.append(make)
    for s in range(1, n):
        last[s - 1]().wait_recv()
        total = total + tot_r[bits + s - 1]
    sum_ref[...] = total

    done = {s: max(0, min(bits - 1, n - 1 - s)) for s in range(1, n)}
    for k in range(bits - 1):
        for s in range(1, n):
            if k >= done[s]:
                level(s, k)
    for s in range(n):
        level(s, bits - 1)

    def project(c, _):
        cols = pl.ds(pl.multiple_of(c * 256, 256), 256)
        out_ref[:, cols] = jnp.dot(
            att[...], w_all[:, cols], preferred_element_type=jnp.float32
        ).astype(out_ref.dtype)
        return 0

    lax.fori_loop(0, width // 256, project, 0)
    for make, cond in sends:
        when(cond, lambda make=make: make().wait_send())


def main_step(q, k, v, docs, cot, w, bits, n):
    tokens = k.shape[0]
    rows, width = w.shape
    half = width // 2
    count = 1 << bits
    skips = reach_skips(tokens, n)
    steps = len(skips)
    sem = pltpu.SemaphoreType.DMA
    vm = pl.BlockSpec(memory_space=pltpu.VMEM)
    pair = HEADS // KV_HEADS
    bf16, f32 = jnp.bfloat16, jnp.float32
    return pl.pallas_call(
        functools.partial(main_kernel, bits, n, skips, 2),
        out_shape=(
            jax.ShapeDtypeStruct((tokens, width), bf16),
            jax.ShapeDtypeStruct((rows, width), f32),
            jax.ShapeDtypeStruct((8, 128), f32),
        ),
        in_specs=[vm] * 6,
        out_specs=(vm,) * 3,
        scratch_shapes=[
            pltpu.VMEM((KV_HEADS, 2, n * tokens, HEAD_DIM), bf16),
            pltpu.VMEM((8, n * tokens), jnp.int32),
            pltpu.VMEM((count * n * rows, width), bf16),
            pltpu.VMEM((tokens, HEADS * HEAD_DIM), bf16),
            pltpu.VMEM((tokens, 128), jnp.int32),
            pltpu.VMEM((pair, tokens, HEAD_DIM), f32),
            pltpu.VMEM((pair, tokens, 1), f32),
            pltpu.VMEM((2, count, n * rows, half), bf16),
            pltpu.VMEM((2, count, n * rows, half), bf16),
            pltpu.VMEM((2, n - 1, rows, half), bf16),
            pltpu.VMEM((2, n - 1, rows, half), bf16),
            pltpu.VMEM((n * rows, width), f32),
            pltpu.VMEM((bits + 1, 8, 128), f32),
            pltpu.VMEM((bits + n - 1, 8, 128), f32),
            sem((2, n - 1)), sem((2, n - 1)),
            sem((steps, KV_HEADS)), sem((steps, KV_HEADS)),
            sem((n - 1,)), sem((n - 1,)),
            sem((n, 2, count)), sem((n, 2, count)),
            sem((2, count)), sem((2, count)),
            sem((2, n - 1)), sem((2, n - 1)),
            sem((bits + n - 1,)), sem((bits + n - 1,)),
        ],
        compiler_params=pltpu.CompilerParams(
            collective_id=0, has_side_effects=True, vmem_limit_bytes=54 * 1024 * 1024
        ),
    )(q, k, v, docs, cot, w)


def adam_kernel(
    entries,
    grad_ref, sum_ref, w_ref, m1_ref, s1_ref, m2_ref, s2_ref,
    nw_ref, n1_ref, ns1_ref, n2_ref, ns2_ref,
    wide1, wide2, tall1, tall2,
):
    rows, width = w_ref.shape
    groups = width // GROUP
    rms = jnp.sqrt(sum_ref[0:1, :] / entries + 1e-06)
    factor = jnp.minimum(1.0, 1.0 / rms)
    for wide, ref in ((wide1, s1_ref), (wide2, s2_ref)):
        wide[...] = jnp.zeros_like(wide)
        wide[0:groups, 0:rows] = ref[...]
    tall1[...] = wide1[...].T
    tall2[...] = wide2[...].T

    def decode(coded, scale):
        x = coded.astype(jnp.float32)
        root = scale * jnp.sqrt(jnp.abs(x))
        return jnp.where(x < 0, -root, root)

    def encode(x):
        scale = jnp.max(jnp.abs(x), axis=-1, keepdims=True) + 1e-06
        return (x * jnp.abs(x) / (scale * scale)).astype(jnp.bfloat16), scale

    for g in range(groups):
        cols = slice(g * GROUP, (g + 1) * GROUP)
        clipped = grad_ref[:, cols] * factor
        first = beta_first * decode(m1_ref[:, cols], tall1[0:rows, g:g + 1]) + (
            1.0 - beta_first
        ) * clipped
        second = (
            beta_second * decode(m2_ref[:, cols], tall2[0:rows, g:g + 1])
            + (1.0 - beta_second) * clipped * clipped
        )
        weight = w_ref[:, cols]
        nw_ref[:, cols] = weight - learn_rate * (
            first / (jnp.sqrt(second) + 1e-08) + decay_rate * weight
        )
        n1_ref[:, cols], tall1[0:rows, g:g + 1] = encode(first)
        n2_ref[:, cols], tall2[0:rows, g:g + 1] = encode(second)
    ns1_ref[...] = tall1[...].T[0:groups, 0:rows]
    ns2_ref[...] = tall2[...].T[0:groups, 0:rows]


def adam(grad, total, weight, m1, s1, m2, s2, entries):
    rows, width = weight.shape
    vm = pl.BlockSpec(memory_space=pltpu.VMEM)
    like = lambda a: jax.ShapeDtypeStruct(a.shape, a.dtype)
    s1, s2 = s1.T, s2.T
    lanes = pl.cdiv(rows, 128) * 128
    deep = pl.cdiv(width // GROUP, 128) * 128
    scratch = [pltpu.VMEM((deep, lanes), jnp.float32)] * 2
    scratch += [pltpu.VMEM((lanes, deep), jnp.float32)] * 2
    nw, n1, ns1, n2, ns2 = pl.pallas_call(
        functools.partial(adam_kernel, entries),
        out_shape=(like(weight), like(m1), like(s1), like(m2), like(s2)),
        in_specs=[vm] * 7,
        out_specs=(vm,) * 5,
        scratch_shapes=scratch,
    )(grad, total, weight, m1, s1, m2, s2)
    return nw, n1, ns1.T, n2, ns2.T


def local(
    bits, n,
    queries, keys, values, segments, cotangent, weight,
    first_moment, first_scale, second_moment, second_scale,
):
    rows, width = weight.shape
    layer_out, grad, total = main_step(
        queries[0], keys[0], values[0],
        segments, cotangent[0], weight, bits, n,
    )
    entries = float((1 << bits) * n * rows * width)
    updated = adam(
        grad, total, weight, first_moment, first_scale, second_moment, second_scale, entries
    )
    return (layer_out[None], *updated)


def solution(mesh):
    bits = mesh.shape["dp"].bit_length() - 1
    n = mesh.shape["seq"]
    shard = P(("dp", "seq"), None)
    tok = P("dp", "seq", None)
    return jax.shard_map(
        functools.partial(local, bits, n),
        mesh=mesh,
        in_specs=(tok, tok, tok, P("dp", "seq"), tok, shard, shard, shard, shard, shard),
        out_specs=(tok, shard, shard, shard, shard, shard),
        check_vma=False,
    )
```

```python
import functools

import jax
import jax.numpy as jnp
from jax import lax
from jax.experimental import pallas as pl
from jax.experimental.pallas import tpu as pltpu
from jax.sharding import PartitionSpec as P

HEADS = 16
KV_HEADS = 8
HEAD_DIM = 128
GROUP = 128

score_scale = 144.0 ** (-0.5)
soft_cap = 50.0
beta_first = 0.9
beta_second = 0.95
learn_rate = 0.001
decay_rate = 0.1

MESH = pl.DeviceIdType.MESH


def longest(length):
    return length * 5 // 8


def reach_skips(tokens, n):
    skips = []
    for s in range(1, n):
        skip = max(0, s * tokens - longest(n * tokens)) // 128 * 128
        if skip < tokens:
            skips.append(skip)
    return tuple(skips)


def orders(bits):
    high = list(range(1, bits))
    return (high, high[::-1])


def flip(me, r):
    out = me
    b = 0
    while (1 << b) <= r:
        if r & (1 << b):
            digit = lax.rem(lax.div(me, 1 << b), 2)
            out = out + (1 - 2 * digit) * (1 << b)
        b += 1
    return out


def greet(me, z, bits, n):
    barrier = pltpu.get_barrier_semaphore()
    for r in range(1, 1 << bits):
        pl.semaphore_signal(
            barrier, inc=1, device_id={"dp": flip(me, r), "seq": z}, device_id_type=MESH
        )
    for s in range(1, n):
        pl.semaphore_signal(
            barrier, inc=1, device_id={"dp": me, "seq": lax.rem(z + s, n)}, device_id_type=MESH
        )
    pl.semaphore_wait(barrier, (1 << bits) + n - 2)


def main_kernel(
    bits, n, skips, ahead,
    q_hbm, k_ref, v_ref, doc_ref, cot_hbm, w_ref,
    out_hbm, own_hbm, sum_ref,
    q_ref, cot_ref, out_ref, own_ref, io_sem, kv_all, doc_all, w_all, att, own_doc, top_doc, acc, tot, q_top, o_top, t_top,
    sb, rb, zs, zr, grad, tot_s, tot_r,
    ws, wr, ks, kr, ds_, dr, ts, tr, bs, br, zss, zsr, qs, qr, hs, hr,
):
    me = lax.axis_index("dp")
    z = lax.axis_index("seq")
    tokens = k_ref.shape[0]
    rows, width = w_ref.shape
    half = width // 2
    big = n * rows
    count = 1 << bits
    per = count // KV_HEADS
    steps = len(skips)
    right, left = lax.rem(z + 1, n), lax.rem(z + n - 1, n)
    group_me = lax.div(me, per)
    sends = []
    load_q = pltpu.make_async_copy(q_hbm, q_ref, io_sem.at[0])
    load_cot = pltpu.make_async_copy(cot_hbm, cot_ref, io_sem.at[1])
    load_q.start()
    load_cot.start()

    def descriptor(src, dst, ssem, rsem, dp, seq):
        return pltpu.make_async_remote_copy(
            src_ref=src, dst_ref=dst, send_sem=ssem, recv_sem=rsem,
            device_id={"dp": dp, "seq": seq}, device_id_type=MESH,
        )

    def go(make, cond=None):
        if cond is None:
            make().start()
        else:

            @pl.when(cond)
            def _():
                make().start()

        sends.append((make, cond))

    def flush(upto):
        now, sends[:] = sends[:upto], sends[upto:]
        while now:
            cond = now[0][1]
            same = 1
            while same < len(now) and now[same][1] is cond:
                same += 1
            batch, now = now[:same], now[same:]

            def act(batch=batch):
                for make, _ in batch:
                    make().wait_send()

            when(cond, act)

    def when(cond, act):
        if cond is None:
            act()
        else:
            pl.when(cond)(act)

    own_rows = pl.ds(pl.multiple_of(z * tokens, 128), tokens)

    def restore_group(g, _):
        cols = pl.ds(pl.multiple_of(g * HEAD_DIM, 128), HEAD_DIM)
        for part, ref in enumerate((k_ref, v_ref)):
            x = ref[:, cols].astype(jnp.float32)
            scale = jnp.max(jnp.abs(x), axis=-1, keepdims=True) + 1e-06
            wide = scale.astype(jnp.bfloat16).astype(jnp.float32)
            coded = (x / wide).astype(jnp.bfloat16).astype(jnp.float32)
            kv_all[g, part, own_rows, :] = (coded * wide).astype(jnp.bfloat16)
        return 0

    lax.fori_loop(0, KV_HEADS, restore_group, 0)
    doc_all[:, own_rows] = jnp.broadcast_to(doc_ref[...], (8, tokens))
    own_doc[...] = jnp.broadcast_to(doc_ref[0:1, :], (128, tokens)).T

    def w_rows(block, zz):
        return pl.ds(pl.multiple_of((block * n + zz) * rows, 16), rows)

    w_all[w_rows(me, z), :] = w_ref[...].astype(jnp.bfloat16)
    for s in range(1, min(steps, n - 2) + 1):
        if skips[s - 1]:

            @pl.when((z >= s) & (z < n - 1))
            def _(s=s):
                stale = pl.ds(pl.multiple_of((z - s) * tokens, 128), skips[s - 1])
                for g in range(KV_HEADS):
                    for part in range(2):
                        kv_all[g, part, stale, :] = jnp.zeros(
                            (skips[s - 1], HEAD_DIM), jnp.bfloat16
                        )

    greet(me, z, bits, n)

    def room(direction, s):
        if direction == 0:
            return (z >= s - 1) & (z < n - 1)
        return (z <= n - s) & (z > 0)

    def landed(direction, s):
        return z >= s if direction == 0 else z <= n - 1 - s

    def group_of(i):
        return flip(group_me, KV_HEADS - 1 - i)

    hops = min(steps, n - 2)
    top = n - 1

    def kv_room(s):
        return (z >= s - 1) & (z < top - 1)

    def kv_landed(s):
        return (z >= s) & (z < top)

    def kv_copy(s, i, at):
        skip = skips[s - 1]
        start = pl.multiple_of(at * tokens + skip, 128)
        part = kv_all.at[group_of(i), :, pl.ds(start, tokens - skip), :]
        return descriptor(part, part, ks.at[s - 1, i], kr.at[s - 1, i], me, right)

    def kv_send(s, i, cond):
        go(lambda: kv_copy(s, i, z - (s - 1)), cond)

    def kv_relay(i):
        for s in range(1, hops + 1):

            @pl.when(kv_landed(s))
            def _(s=s):
                kv_copy(s, i, z - s).wait_recv()

            if s < hops:
                kv_send(s + 1, i, kv_room(s + 1))

    def w_hop(direction, s, at):
        part = w_all.at[w_rows(me, at), :]
        return descriptor(
            part, part, ws.at[direction, s - 1], wr.at[direction, s - 1],
            me, right if direction == 0 else left,
        )

    def w_send(direction, s, cond=None):
        at = z - (s - 1) if direction == 0 else z + (s - 1)
        cond = room(direction, s) if cond is None else cond
        go(lambda: w_hop(direction, s, at), cond)

    w_tree = [list(order) + [0] for order in orders(bits)]
    w_stage = []
    for h in range(2):
        seen, levels = [0], []
        for b in w_tree[h]:
            fresh = [r | (1 << b) for r in seen]
            levels.append(fresh)
            seen = seen + fresh
        w_stage.append(levels)

    def w_forward(zz, h, r, cond):
        order = w_tree[h]
        last = -1
        for i, b in enumerate(order):
            if r & (1 << b):
                last = i
        for b in order[last + 1:]:
            nr = r | (1 << b)

            def make(b=b, nr=nr):
                part = w_all.at[w_rows(flip(me, r), zz), pl.ds(h * half, half)]
                return descriptor(
                    part, part, ts.at[zz, h, nr], tr.at[zz, h, nr], flip(me, 1 << b), z
                )

            go(make, cond)

    def w_wait(zz, h, r, cond):
        def act():
            part = w_all.at[w_rows(flip(me, r), zz), pl.ds(h * half, half)]
            descriptor(part, part, ts.at[zz, h, r], tr.at[zz, h, r], me, right).wait_recv()

        when(cond, act)

    def w_level(zz, level, cond):
        for j in range(len(w_stage[0][level])):
            for h in range(2):
                r = w_stage[h][level][j]
                w_wait(zz, h, r, cond)
                if level < bits - 1:
                    w_forward(zz, h, r, cond)

    def source(direction, s):
        return z - s if direction == 0 else z + s

    def source(direction, s):
        return z - s if direction == 0 else z + s

    def land(direction, s, cond):
        @pl.when(cond)
        def _():
            w_hop(direction, s, source(direction, s)).wait_recv()

    def spread(direction, s, cond):
        for h in range(2):
            w_forward(source(direction, s), h, 0, cond)

    def level(direction, s, k, cond=None):
        if s == 0:
            w_level(z, k, None)
        else:
            cond = landed(direction, s) if cond is None else cond
            w_level(source(direction, s), k, cond)

    events = {i: [] for i in range(KV_HEADS)}

    def plan(i, act):
        events[min(i, KV_HEADS - 1)].append(act)

    chunks = []

    def chunk(direction, s, cond, lands=None, spreads=None, sees=()):
        item = {"at": (direction, s, cond), "done": 0, "landed": False, "here": False}
        chunks.append(item)

        def touch():
            land(direction, s, cond)
            item["landed"] = True

        def come():
            if not item["landed"]:
                touch()
            spread(direction, s, cond)
            item["here"] = True

        def deeper():
            level(direction, s, item["done"], cond)
            item["done"] += 1

        item["come"], item["deeper"] = come, deeper
        if lands is not None:
            plan(lands, touch)
        if spreads is not None:
            plan(spreads, come)
        for i in sees[:bits - 1]:
            plan(i, deeper)

    def turn():
        for item in chunks:
            if item["here"] and item["done"] < bits - 1:
                item["deeper"]()

    at_top, helper, below = z == top, z == top - 1, (z > 0) & (z < top - 1)
    for k in range(bits - 1):
        plan(2 * k, lambda k=k: level(0, 0, k))
    chunk(1, 1, landed(1, 1), 1, 2, (7,))
    chunk(0, 1, at_top, None, 0, (1, 3))
    chunk(0, 1, helper & (z > 0), 0, 2, (7,))
    chunk(0, 1, below, None, 7)
    if n > 2:
        plan(1, lambda: w_send(1, 2))
        plan(0, lambda: w_send(0, 2, helper & (z > 0)))
        plan(7, lambda: w_send(0, 2, below))
        chunk(0, 2, at_top, None, 1, (4, 7))
        chunk(1, 2, landed(1, 2), 7, 7)
        chunk(0, 2, landed(0, 2) & (z < top))
    if n > 3:
        plan(7, lambda: w_send(1, 3))
    for s in range(3, n):
        chunk(0, s, landed(0, s))
        chunk(1, s, landed(1, s))

    pair = HEADS // KV_HEADS
    span = pair * HEAD_DIM

    def q_cols(i):
        return pl.ds(pl.multiple_of(group_of(i) * span, 128), span)

    def q_copy(i):
        return descriptor(
            q_ref.at[:, q_cols(i)], q_top.at[i], hs.at[0, i], hr.at[0, i], me, left
        )

    def o_copy(i):
        return descriptor(
            o_top.at[i], o_top.at[i], hs.at[1, i], hr.at[1, i], me, right
        )

    def t_copy(i):
        return descriptor(
            t_top.at[i], t_top.at[i], hs.at[2, i], hr.at[2, i], me, right
        )

    load_q.wait()
    doc_copies = []
    for s in range(1, n):
        def make(s=s):
            slot = doc_all.at[:, own_rows]
            return descriptor(
                slot, slot, ds_.at[s - 1], dr.at[s - 1], me, lax.rem(z + s, n)
            )

        go(make)
        doc_copies.append(make)
    for i in range(KV_HEADS):
        if hops:
            kv_send(1, i, kv_room(1) if i < ahead else (z == 0) & kv_room(1))
        go(lambda i=i: q_copy(i), z == top)
        if i == 0:
            w_send(0, 1, (z > 0) & (z < top))
        if i == 1:
            w_send(1, 1)
            w_send(0, 1, (z == 0) & (z < top))
    for h in range(2):
        w_forward(z, h, 0, None)

    query_at = lax.broadcasted_iota(jnp.int32, (tokens, tokens), 0)
    key_at = lax.broadcasted_iota(jnp.int32, (tokens, tokens), 1)
    lo = jnp.where(z == top, z, jnp.maximum(z - steps, 0))

    def blocks(g, query, docs_ref, at_block, first, stop):
        acc[...] = jnp.zeros_like(acc)
        tot[...] = jnp.zeros_like(tot)

        def block(j, _):
            at = pl.ds(pl.multiple_of(j * tokens, 128), tokens)
            same = docs_ref[:, 0:1] == doc_all[0:1, at]
            allowed = same & (key_at + (j - at_block) * tokens <= query_at)
            key = kv_all[g, 0, at, :]
            value = kv_all[g, 1, at, :]
            for hd in range(pair):
                scores = lax.dot_general(
                    query(hd), key, (((1,), (1,)), ((), ())),
                    preferred_element_type=jnp.float32,
                )
                capped = soft_cap * jnp.tanh(scores * (score_scale / soft_cap))
                weights = jnp.where(allowed, jnp.exp(capped), 0.0)
                tot[hd] = tot[hd] + jnp.sum(weights, axis=-1, keepdims=True)
                acc[hd] = acc[hd] + jnp.dot(
                    weights.astype(jnp.bfloat16), value, preferred_element_type=jnp.float32
                )
            return 0

        lax.fori_loop(first, stop, block, 0)

    def attend_for_top(i):
        g = group_of(i)
        q_copy(i).wait_recv()
        blocks(
            g, lambda hd: q_top[i, :, hd * HEAD_DIM:(hd + 1) * HEAD_DIM],
            top_doc, top, max(top - steps, 0), top,
        )
        for hd in range(pair):
            o_top[i, :, hd * HEAD_DIM:(hd + 1) * HEAD_DIM] = acc[hd].astype(jnp.bfloat16)
            line = jnp.broadcast_to(tot[hd], (tokens, 128)).T
            t_top[i, hd * 4:(hd + 1) * 4, :] = line[0:4, :]
        o_copy(i).start()
        t_copy(i).start()

    def attend_group(i):
        g = group_of(i)

        def query(hd):
            return q_ref[:, pl.ds(pl.multiple_of((g * pair + hd) * HEAD_DIM, 128), HEAD_DIM)]

        blocks(g, query, own_doc, z, lo, z + 1)

        @pl.when(z == top)
        def _():
            o_copy(i).wait_recv()
            t_copy(i).wait_recv()
            for hd in range(pair):
                part = o_top[i, :, hd * HEAD_DIM:(hd + 1) * HEAD_DIM]
                acc[hd] = acc[hd] + part.astype(jnp.float32)
                line = t_top[i, hd * 4:hd * 4 + 1, :]
                tot[hd] = tot[hd] + jnp.broadcast_to(line, (128, tokens)).T[:, 0:1]

        for hd in range(pair):
            cols = pl.ds(pl.multiple_of((g * pair + hd) * HEAD_DIM, 128), HEAD_DIM)
            att[:, cols] = (acc[hd] / tot[hd]).astype(att.dtype)

    tree = [[0] + list(order) for order in orders(bits)]

    def first_bit(r, h):
        for b in tree[h]:
            if r & (1 << b):
                return b

    def sources(r, h):
        out = []
        for b in tree[h]:
            if r & (1 << b):
                break
            out.append(r | (1 << b))
        return out

    def block_t(r):
        start = pl.multiple_of(flip(me, r) * big, 128)
        return att[:, pl.ds(start, big)].T

    def reduce_block(r, h, block):
        value = jnp.dot(
            block, cot_ref[:, h * half:(h + 1) * half], preferred_element_type=jnp.float32
        )
        for src in sources(r, h):
            descriptor(
                sb.at[h, src], rb.at[h, src], bs.at[h, src], br.at[h, src], me, right
            ).wait_recv()
            value = value + rb[h, src].astype(jnp.float32)
        if r == 0:
            grad[:, h * half:(h + 1) * half] = value
            return
        sb[h, r] = value.astype(jnp.bfloat16)
        b = first_bit(r, h)
        go(lambda: descriptor(
            sb.at[h, r], rb.at[h, r], bs.at[h, r], br.at[h, r], flip(me, 1 << b), z
        ))

    late = []
    for i in range(KV_HEADS):
        if i == KV_HEADS // 2:
            early = len(sends)
        kv_relay(i)
        if hops and i + ahead < KV_HEADS:
            kv_send_next = i + ahead
            go(
                lambda j=kv_send_next: kv_copy(1, j, z), (z > 0) & kv_room(1)
            )
        for act in events[i]:
            act()
        if i == 0:
            load_cot.wait()
            for make in doc_copies:
                make().wait_recv()
            line = doc_all[0:1, top * tokens:(top + 1) * tokens]
            top_doc[...] = jnp.broadcast_to(line, (128, tokens)).T

        @pl.when(z == top - 1)
        def _():
            attend_for_top(i)

        attend_group(i)
        for r, h in late:
            reduce_block(r, h, block_t(r))
        late = []
        for r in range((KV_HEADS - i) * per - 1, (KV_HEADS - 1 - i) * per - 1, -1):
            if r == 0:
                continue
            block = block_t(r)
            for h in range(2):
                if len(sources(r, h)) > 1 and i < 4:
                    late.append((r, h))
                else:
                    reduce_block(r, h, block)

    lanes = (half // 128 + 1) // 2 * 128

    def ring_step(h, s):
        for direction in range(2):
            cut = slice(0, lanes) if direction == 0 else slice(lanes, half)
            cols = slice(h * half + cut.start, h * half + cut.stop)
            wide = cut.stop - cut.start
            q = 2 * h + direction
            shift = (2 * n - 1 - s) if direction == 0 else (1 + s)
            at = lax.rem(z + shift, n)

            def make(s, q=q, wide=wide, direction=direction):
                return descriptor(
                    zs.at[q, s, :, 0:wide], zr.at[q, s, :, 0:wide],
                    zss.at[q, s], zsr.at[q, s], me, right if direction == 0 else left,
                )

            value = grad[pl.ds(pl.multiple_of(at * rows, 16), rows), cols]
            if s:
                make(s - 1).wait_recv()
                value = value + zr[q, s - 1, :, 0:wide].astype(jnp.float32)
            if s < n - 1:
                zs[q, s, :, 0:wide] = value.astype(jnp.bfloat16)
                go(lambda make=make: make(s))
            else:
                own_ref[:, cols] = value

    def tail_arrive(s):
        for item in chunks:
            if item["at"][1] == s and not item["here"]:
                item["come"]()
        if s + 1 < n:
            w_send(0, s + 1)
            if s >= 3:
                w_send(1, s + 1)

    if n > 2:
        tail_arrive(2)
    last_block = block_t(0)
    reduce_block(0, 0, last_block)
    ring_step(0, 0)
    middle = len(sends) - early
    flush(early)
    ring_step(0, 1)
    reduce_block(0, 1, last_block)
    ring_step(1, 0)
    if n > 3:
        tail_arrive(3)
    flush(middle)

    @pl.when(z == top - 1)
    def _():
        for i in range(KV_HEADS):
            o_copy(i).wait_send()
            t_copy(i).wait_send()

    for s in range(2, n + 1):
        if s < n:
            ring_step(0, s)
        turn()
        ring_step(1, s - 1)
        if s + 2 < n:
            tail_arrive(s + 2)

    own = own_ref[...]
    save_own = pltpu.make_async_copy(own_ref, own_hbm, io_sem.at[2])
    save_own.start()
    total = jnp.broadcast_to(
        jnp.sum(jnp.sum(own * own, axis=1, keepdims=True), axis=0, keepdims=True), (8, 128)
    )
    for k in range(bits - 1):
        turn()

    def project(c, _):
        cols = pl.ds(pl.multiple_of(c * 256, 256), 256)
        out_ref[:, cols] = jnp.dot(
            att[...], w_all[:, cols], preferred_element_type=jnp.float32
        ).astype(out_ref.dtype)
        return 0

    tiles = width // 256
    mid = tiles // 2 * 256

    def save(cut, i):
        return pltpu.make_async_copy(out_ref.at[:, cut], out_hbm.at[:, cut], io_sem.at[i])

    save_left, save_right = save(slice(0, mid), 3), save(slice(mid, width), 4)
    stage = [
        [(r, flip(me, r), z) for r in range(1, count)],
        [(count + s - 1, me, lax.rem(z + s, n)) for s in range(1, n)],
    ]
    for j, peers in enumerate(stage):
        tot_s[j] = total
        for i, dp, seq in peers:
            go(lambda i=i, dp=dp, seq=seq, j=j: descriptor(
                tot_s.at[j], tot_r.at[i], qs.at[i], qr.at[i], dp, seq
            ))
        if j == 0:
            level(0, 0, bits - 1)
            for s in range(1, n):
                for direction in range(2):
                    level(direction, s, bits - 1)
            lax.fori_loop(0, tiles // 2, project, 0)
            save_left.start()
        else:
            lax.fori_loop(tiles // 2, tiles, project, 0)
            save_right.start()
        for i, dp, seq in peers:
            descriptor(
                tot_s.at[j], tot_r.at[i], qs.at[i], qr.at[i], dp, seq
            ).wait_recv()
            total = total + tot_r[i]
    sum_ref[...] = total
    flush(len(sends))
    save_own.wait()
    save_left.wait()
    save_right.wait()


def main_step(q, k, v, docs, cot, w, bits, n):
    tokens = k.shape[0]
    rows, width = w.shape
    half = width // 2
    count = 1 << bits
    skips = reach_skips(tokens, n)
    steps = len(skips)
    lanes = (half // 128 + 1) // 2 * 128
    sem = pltpu.SemaphoreType.DMA
    vm = pl.BlockSpec(memory_space=pltpu.VMEM)
    hbm = pl.BlockSpec(memory_space=pl.ANY)
    pair = HEADS // KV_HEADS
    bf16, f32 = jnp.bfloat16, jnp.float32
    return pl.pallas_call(
        functools.partial(main_kernel, bits, n, skips, 2),
        out_shape=(
            jax.ShapeDtypeStruct((tokens, width), bf16),
            jax.ShapeDtypeStruct((rows, width), f32),
            jax.ShapeDtypeStruct((8, 128), f32),
        ),
        in_specs=[hbm, vm, vm, vm, hbm, vm],
        out_specs=(hbm, hbm, vm),
        scratch_shapes=[
            pltpu.VMEM(q.shape, q.dtype),
            pltpu.VMEM(cot.shape, cot.dtype),
            pltpu.VMEM((tokens, width), bf16),
            pltpu.VMEM((rows, width), f32),
            sem((5,)),
            pltpu.VMEM((KV_HEADS, 2, n * tokens, HEAD_DIM), bf16),
            pltpu.VMEM((8, n * tokens), jnp.int32),
            pltpu.VMEM((count * n * rows, width), bf16),
            pltpu.VMEM((tokens, HEADS * HEAD_DIM), bf16),
            pltpu.VMEM((tokens, 128), jnp.int32),
            pltpu.VMEM((tokens, 128), jnp.int32),
            pltpu.VMEM((pair, tokens, HEAD_DIM), f32),
            pltpu.VMEM((pair, tokens, 1), f32),
            pltpu.VMEM((KV_HEADS, tokens, pair * HEAD_DIM), bf16),
            pltpu.VMEM((KV_HEADS, tokens, pair * HEAD_DIM), bf16),
            pltpu.VMEM((KV_HEADS, 8, tokens), f32),
            pltpu.VMEM((2, count, n * rows, half), bf16),
            pltpu.VMEM((2, count, n * rows, half), bf16),
            pltpu.VMEM((4, n - 1, rows, lanes), bf16),
            pltpu.VMEM((4, n - 1, rows, lanes), bf16),
            pltpu.VMEM((n * rows, width), f32),
            pltpu.VMEM((2, 8, 128), f32),
            pltpu.VMEM((count + n - 1, 8, 128), f32),
            sem((2, n - 1)), sem((2, n - 1)),
            sem((steps, KV_HEADS)), sem((steps, KV_HEADS)),
            sem((n - 1,)), sem((n - 1,)),
            sem((n, 2, count)), sem((n, 2, count)),
            sem((2, count)), sem((2, count)),
            sem((4, n - 1)), sem((4, n - 1)),
            sem((count + n - 1,)), sem((count + n - 1,)),
            sem((3, KV_HEADS)), sem((3, KV_HEADS)),
        ],
        compiler_params=pltpu.CompilerParams(
            collective_id=0, has_side_effects=True, vmem_limit_bytes=54 * 1024 * 1024
        ),
    )(q, k, v, docs, cot, w)


def adam_kernel(
    entries, tile,
    grad_ref, sum_ref, w_ref, m1_ref, s1_ref, m2_ref, s2_ref, layer_ref,
    nw_ref, n1_ref, ns1_ref, n2_ref, ns2_ref, layer_out_ref,
    wide, tall1, tall2, out1, out2, hold, sem,
):
    step = pl.program_id(0)
    take = pltpu.make_async_copy(layer_ref, hold, sem.at[0])
    give = pltpu.make_async_copy(hold, layer_out_ref, sem.at[1])

    @pl.when(step == 0)
    def _():
        take.start()

    @pl.when(step == 1)
    def _():
        take.wait()
        give.start()

    rows = w_ref.shape[0]
    groups = s1_ref.shape[0]
    rms = jnp.sqrt(sum_ref[0:1, :] / entries + 1e-06)
    factor = jnp.minimum(1.0, 1.0 / rms)
    lane = lax.broadcasted_iota(jnp.int32, tall1.shape, 1)

    @pl.when(step == 0)
    def _():
        for tall, ref in ((tall1, s1_ref), (tall2, s2_ref)):
            wide[...] = jnp.zeros_like(wide)
            wide[0:groups, 0:rows] = ref[...]
            tall[...] = wide[...].T

    def decode(coded, tall, g):
        x = coded.astype(jnp.float32)
        scale = jnp.sum(jnp.where(lane == g, tall[...], 0.0), axis=-1, keepdims=True)[0:rows]
        root = scale * jnp.sqrt(jnp.abs(x))
        return jnp.where(x < 0, -root, root)

    def encode(x, out, g):
        scale = jnp.max(jnp.abs(x), axis=-1, keepdims=True) + 1e-06
        out[0:rows] = jnp.where(lane[0:rows] == g, scale, out[0:rows])
        return (x * jnp.abs(x) / (scale * scale)).astype(jnp.bfloat16)

    for j in range(tile // GROUP):
        g = step * (tile // GROUP) + j
        cols = slice(j * GROUP, (j + 1) * GROUP)
        clipped = grad_ref[:, cols] * factor
        first = beta_first * decode(m1_ref[:, cols], tall1, g) + (
            1.0 - beta_first
        ) * clipped
        second = (
            beta_second * decode(m2_ref[:, cols], tall2, g)
            + (1.0 - beta_second) * clipped * clipped
        )
        weight = w_ref[:, cols]
        nw_ref[:, cols] = weight - learn_rate * (
            first / (jnp.sqrt(second) + 1e-08) + decay_rate * weight
        )
        n1_ref[:, cols] = encode(first, out1, g)
        n2_ref[:, cols] = encode(second, out2, g)

    @pl.when(step == pl.num_programs(0) - 1)
    def _():
        ns1_ref[...] = out1[...].T[0:groups, 0:rows]
        ns2_ref[...] = out2[...].T[0:groups, 0:rows]
        give.wait()


def adam(layer, grad, total, weight, m1, s1, m2, s2, entries):
    rows, width = weight.shape
    like = lambda a: jax.ShapeDtypeStruct(a.shape, a.dtype)
    s1, s2 = s1.T, s2.T
    lanes = pl.cdiv(rows, 128) * 128
    deep = pl.cdiv(width // GROUP, 128) * 128
    parts = 3
    tile = width // parts
    cut = pl.BlockSpec((rows, tile), lambda i: (0, i))
    whole = lambda a: pl.BlockSpec(a.shape, lambda i: (0, 0))
    scratch = [pltpu.VMEM((deep, lanes), jnp.float32)]
    scratch += [pltpu.VMEM((lanes, deep), jnp.float32)] * 4
    scratch += [pltpu.VMEM(layer.shape, layer.dtype), pltpu.SemaphoreType.DMA((2,))]
    far = pl.BlockSpec(memory_space=pl.ANY)
    nw, n1, ns1, n2, ns2, layer = pl.pallas_call(
        functools.partial(adam_kernel, entries, tile),
        grid=(parts,),
        out_shape=(like(weight), like(m1), like(s1), like(m2), like(s2), like(layer)),
        in_specs=[cut, whole(total), cut, cut, whole(s1), cut, whole(s2), far],
        out_specs=(cut, cut, whole(s1), cut, whole(s2), far),
        scratch_shapes=scratch,
    )(grad, total, weight, m1, s1, m2, s2, layer)
    return layer, nw, n1, ns1.T, n2, ns2.T


def local(
    bits, n,
    queries, keys, values, segments, cotangent, weight,
    first_moment, first_scale, second_moment, second_scale,
):
    rows, width = weight.shape
    layer_out, grad, total = main_step(
        queries[0], keys[0], values[0],
        segments, cotangent[0], weight, bits, n,
    )
    entries = float((1 << bits) * n * rows * width)
    layer_out, *updated = adam(
        layer_out, grad, total, weight,
        first_moment, first_scale, second_moment, second_scale, entries,
    )
    return (layer_out[None], *updated)


def solution(mesh):
    bits = mesh.shape["dp"].bit_length() - 1
    n = mesh.shape["seq"]
    shard = P(("dp", "seq"), None)
    tok = P("dp", "seq", None)
    return jax.shard_map(
        functools.partial(local, bits, n),
        mesh=mesh,
        in_specs=(tok, tok, tok, P("dp", "seq"), tok, shard, shard, shard, shard, shard),
        out_specs=(tok, shard, shard, shard, shard, shard),
        check_vma=False,
    )
```

```python
import functools

import jax
import jax.numpy as jnp
from jax import lax
from jax.experimental import pallas as pl
from jax.experimental.pallas import tpu as pltpu
from jax.sharding import PartitionSpec as P

HEADS = 16
KV_HEADS = 8
HEAD_DIM = 128
GROUP = 128

score_scale = 144.0 ** (-0.5)
soft_cap = 50.0
beta_first = 0.9
beta_second = 0.95
learn_rate = 0.001
decay_rate = 0.1

MESH = pl.DeviceIdType.MESH


def longest(length):
    return length * 5 // 8


def reach_skips(tokens, n):
    skips = []
    for s in range(1, n):
        skip = max(0, s * tokens - longest(n * tokens)) // 128 * 128
        if skip < tokens:
            skips.append(skip)
    return tuple(skips)


def orders(bits):
    high = list(range(1, bits))
    return (high, high[::-1])


def flip(me, r):
    out = me
    b = 0
    while (1 << b) <= r:
        if r & (1 << b):
            digit = lax.rem(lax.div(me, 1 << b), 2)
            out = out + (1 - 2 * digit) * (1 << b)
        b += 1
    return out


def greet(me, z, bits, n):
    barrier = pltpu.get_barrier_semaphore()
    for r in range(1, 1 << bits):
        pl.semaphore_signal(
            barrier, inc=1, device_id={"dp": flip(me, r), "seq": z}, device_id_type=MESH
        )
    for s in range(1, n):
        pl.semaphore_signal(
            barrier, inc=1, device_id={"dp": me, "seq": lax.rem(z + s, n)}, device_id_type=MESH
        )
    pl.semaphore_wait(barrier, (1 << bits) + n - 2)


def main_kernel(
    bits, n, skips, ahead,
    q_hbm, k_ref, v_ref, doc_ref, cot_hbm, w_ref,
    out_hbm, own_hbm, sum_ref,
    q_ref, cot_ref, out_ref, own_ref, io_sem, kv_all, doc_all, w_all, att, own_doc, top_doc, acc, tot, q_top, o_top, t_top,
    sb, rb, zs, zr, grad, extra, own_extra, x_s, x_r, tot_s, tot_r,
    ws, wr, ks, kr, ds_, dr, ts, tr, bs, br, zss, zsr, qs, qr, hs, hr, xs,
):
    me = lax.axis_index("dp")
    z = lax.axis_index("seq")
    tokens = k_ref.shape[0]
    rows, width = w_ref.shape
    half = width // 2
    big = n * rows
    count = 1 << bits
    per = count // KV_HEADS
    steps = len(skips)
    right, left = lax.rem(z + 1, n), lax.rem(z + n - 1, n)
    group_me = lax.div(me, per)
    sends = []
    load_q = pltpu.make_async_copy(q_hbm, q_ref, io_sem.at[0])
    load_cot = pltpu.make_async_copy(cot_hbm, cot_ref, io_sem.at[1])
    load_q.start()
    load_cot.start()

    def descriptor(src, dst, ssem, rsem, dp, seq):
        return pltpu.make_async_remote_copy(
            src_ref=src, dst_ref=dst, send_sem=ssem, recv_sem=rsem,
            device_id={"dp": dp, "seq": seq}, device_id_type=MESH,
        )

    def go(make, cond=None, keep=True):
        if cond is None:
            make().start()
        else:

            @pl.when(cond)
            def _():
                make().start()

        if keep:
            sends.append((make, cond))

    def sent(ref, sem):
        descriptor(ref, ref, sem, sem, me, right).wait_send()

    def flush(upto):
        now, sends[:] = sends[:upto], sends[upto:]
        while now:
            cond = now[0][1]
            same = 1
            while same < len(now) and now[same][1] is cond:
                same += 1
            batch, now = now[:same], now[same:]

            def act(batch=batch):
                for make, _ in batch:
                    make().wait_send()

            when(cond, act)

    def when(cond, act):
        if cond is None:
            act()
        else:
            pl.when(cond)(act)

    own_rows = pl.ds(pl.multiple_of(z * tokens, 128), tokens)

    def restore_group(g, _):
        cols = pl.ds(pl.multiple_of(g * HEAD_DIM, 128), HEAD_DIM)
        for part, ref in enumerate((k_ref, v_ref)):
            x = ref[:, cols].astype(jnp.float32)
            scale = jnp.max(jnp.abs(x), axis=-1, keepdims=True) + 1e-06
            wide = scale.astype(jnp.bfloat16).astype(jnp.float32)
            coded = (x / wide).astype(jnp.bfloat16).astype(jnp.float32)
            kv_all[g, part, own_rows, :] = (coded * wide).astype(jnp.bfloat16)
        return 0

    lax.fori_loop(0, KV_HEADS, restore_group, 0)
    doc_all[:, own_rows] = jnp.broadcast_to(doc_ref[...], (8, tokens))
    own_doc[...] = jnp.broadcast_to(doc_ref[0:1, :], (128, tokens)).T

    def w_rows(block, zz):
        return pl.ds(pl.multiple_of((block * n + zz) * rows, 16), rows)

    w_all[w_rows(me, z), :] = w_ref[...].astype(jnp.bfloat16)
    for s in range(1, min(steps, n - 2) + 1):
        if skips[s - 1]:

            @pl.when((z >= s) & (z < n - 1))
            def _(s=s):
                stale = pl.ds(pl.multiple_of((z - s) * tokens, 128), skips[s - 1])
                for g in range(KV_HEADS):
                    for part in range(2):
                        kv_all[g, part, stale, :] = jnp.zeros(
                            (skips[s - 1], HEAD_DIM), jnp.bfloat16
                        )

    greet(me, z, bits, n)

    def room(direction, s):
        if direction == 0:
            return (z >= s - 1) & (z < n - 1)
        return (z <= n - s) & (z > 0)

    def landed(direction, s):
        return z >= s if direction == 0 else z <= n - 1 - s

    def group_of(i):
        return flip(group_me, KV_HEADS - 1 - i)

    hops = min(steps, n - 2)
    top = n - 1

    def kv_room(s):
        return (z >= s - 1) & (z < top - 1)

    def kv_landed(s):
        return (z >= s) & (z < top)

    def kv_copy(s, i, at):
        skip = skips[s - 1]
        start = pl.multiple_of(at * tokens + skip, 128)
        part = kv_all.at[group_of(i), :, pl.ds(start, tokens - skip), :]
        return descriptor(part, part, ks.at[s - 1], kr.at[s - 1, i], me, right)

    def kv_send(s, i, cond):
        go(lambda: kv_copy(s, i, z - (s - 1)), cond, False)

    def kv_relay(i):
        for s in range(1, hops + 1):

            @pl.when(kv_landed(s))
            def _(s=s):
                kv_copy(s, i, z - s).wait_recv()

            if s < hops:
                kv_send(s + 1, i, kv_room(s + 1))

    def w_hop(direction, s, at):
        part = w_all.at[w_rows(me, at), :]
        return descriptor(
            part, part, ws.at[direction, s - 1], wr.at[direction, s - 1],
            me, right if direction == 0 else left,
        )

    def w_send(direction, s, cond=None):
        at = z - (s - 1) if direction == 0 else z + (s - 1)
        cond = room(direction, s) if cond is None else cond
        go(lambda: w_hop(direction, s, at), cond)

    w_tree = [list(order) + [0] for order in orders(bits)]
    w_stage = []
    for h in range(2):
        seen, levels = [0], []
        for b in w_tree[h]:
            fresh = [r | (1 << b) for r in seen]
            levels.append(fresh)
            seen = seen + fresh
        w_stage.append(levels)

    def w_sem(zz, h, r):
        return ts.at[1] if r % 2 else tr.at[zz, h, r // 2]

    def w_forward(zz, h, r, cond):
        order = w_tree[h]
        last = -1
        for i, b in enumerate(order):
            if r & (1 << b):
                last = i
        for b in order[last + 1:]:
            nr = r | (1 << b)

            def make(b=b, nr=nr):
                part = w_all.at[w_rows(flip(me, r), zz), pl.ds(h * half, half)]
                return descriptor(
                    part, part, ts.at[0], w_sem(zz, h, nr), flip(me, 1 << b), z
                )

            go(make, cond, False)

    def w_wait(zz, h, r, cond):
        def act():
            part = w_all.at[w_rows(flip(me, r), zz), pl.ds(h * half, half)]
            descriptor(part, part, ts.at[0], w_sem(zz, h, r), me, right).wait_recv()

        when(cond, act)

    def w_level(zz, level, cond):
        for j in range(len(w_stage[0][level])):
            for h in range(2):
                r = w_stage[h][level][j]
                w_wait(zz, h, r, cond)
                if level < bits - 1:
                    w_forward(zz, h, r, cond)

    def source(direction, s):
        return z - s if direction == 0 else z + s

    def source(direction, s):
        return z - s if direction == 0 else z + s

    def land(direction, s, cond):
        @pl.when(cond)
        def _():
            w_hop(direction, s, source(direction, s)).wait_recv()

    def spread(direction, s, cond):
        for h in range(2):
            w_forward(source(direction, s), h, 0, cond)

    def level(direction, s, k, cond=None):
        if s == 0:
            w_level(z, k, None)
        else:
            cond = landed(direction, s) if cond is None else cond
            w_level(source(direction, s), k, cond)

    events = {i: [] for i in range(KV_HEADS)}

    def plan(i, act):
        events[min(i, KV_HEADS - 1)].append(act)

    chunks = []

    def chunk(direction, s, cond, lands=None, spreads=None, sees=(), soon=False):
        item = {"at": (direction, s, cond), "done": 0, "landed": False, "here": False, "soon": soon}
        chunks.append(item)

        def touch():
            land(direction, s, cond)
            item["landed"] = True

        def come():
            if not item["landed"]:
                touch()
            spread(direction, s, cond)
            item["here"] = True

        def deeper():
            level(direction, s, item["done"], cond)
            item["done"] += 1

        item["come"], item["deeper"] = come, deeper
        if lands is not None:
            plan(lands, touch)
        if spreads is not None:
            plan(spreads, come)
        for i in sees[:bits - 1]:
            plan(i, deeper)

    def turn(soon=False):
        for item in chunks:
            if soon and not item["soon"]:
                continue
            if item["here"] and item["done"] < bits - 1:
                item["deeper"]()

    at_top, helper, below = z == top, z == top - 1, (z > 0) & (z < top - 1)
    for k in range(bits - 1):
        plan(2 * k, lambda k=k: level(0, 0, k))
    chunk(1, 1, landed(1, 1), 1, 2, (7,))
    chunk(0, 1, at_top, None, 0, (1, 3))
    chunk(0, 1, helper & (z > 0), 0, 5, ())
    chunk(0, 1, below, None, 7, soon=True)
    if n > 2:
        plan(1, lambda: w_send(1, 2))
        plan(0, lambda: w_send(0, 2, helper & (z > 0)))
        plan(7, lambda: w_send(0, 2, below))
        chunk(0, 2, at_top, None, 1, (4,), soon=True)
        chunk(1, 2, landed(1, 2), 7, 7, soon=True)
        chunk(0, 2, landed(0, 2) & (z < top))
    if n > 3:
        plan(7, lambda: w_send(1, 3))
    for s in range(3, n):
        chunk(0, s, landed(0, s))
        chunk(1, s, landed(1, s))

    pair = HEADS // KV_HEADS
    span = pair * HEAD_DIM

    def q_cols(i):
        return pl.ds(pl.multiple_of(group_of(i) * span, 128), span)

    def q_copy(i):
        return descriptor(
            q_ref.at[:, q_cols(i)], q_top.at[i], hs.at[0], hr.at[0, i], me, left
        )

    def o_copy(i):
        return descriptor(
            o_top.at[i], o_top.at[i], hs.at[1], hr.at[1, i], me, right
        )

    def t_copy(i):
        return descriptor(
            t_top.at[i], t_top.at[i], hs.at[2], hr.at[2, i], me, right
        )

    load_q.wait()
    doc_copies = []
    for s in range(1, n):
        def make(s=s):
            slot = doc_all.at[:, own_rows]
            return descriptor(
                slot, slot, ds_.at[0], dr.at[s - 1], me, lax.rem(z + s, n)
            )

        go(make, None, False)
        doc_copies.append(make)
    for i in range(KV_HEADS):
        if hops:
            kv_send(1, i, kv_room(1) if i < ahead else (z == 0) & kv_room(1))
        go(lambda i=i: q_copy(i), z == top, False)
        if i == 0:
            w_send(0, 1, (z > 0) & (z < top))
        if i == 1:
            w_send(1, 1)
            w_send(0, 1, (z == 0) & (z < top))
    for h in range(2):
        w_forward(z, h, 0, None)

    query_at = lax.broadcasted_iota(jnp.int32, (tokens, tokens), 0)
    key_at = lax.broadcasted_iota(jnp.int32, (tokens, tokens), 1)
    lo = jnp.where(z == top, z, jnp.maximum(z - steps, 0))

    def blocks(g, query, docs_ref, at_block, first, stop):
        acc[...] = jnp.zeros_like(acc)
        tot[...] = jnp.zeros_like(tot)

        def block(j, _):
            at = pl.ds(pl.multiple_of(j * tokens, 128), tokens)
            same = docs_ref[:, 0:1] == doc_all[0:1, at]
            allowed = same & (key_at + (j - at_block) * tokens <= query_at)
            key = kv_all[g, 0, at, :]
            value = kv_all[g, 1, at, :]
            for hd in range(pair):
                scores = lax.dot_general(
                    query(hd), key, (((1,), (1,)), ((), ())),
                    preferred_element_type=jnp.float32,
                )
                capped = soft_cap * jnp.tanh(scores * (score_scale / soft_cap))
                weights = jnp.where(allowed, jnp.exp(capped), 0.0)
                tot[hd] = tot[hd] + jnp.sum(weights, axis=-1, keepdims=True)
                acc[hd] = acc[hd] + jnp.dot(
                    weights.astype(jnp.bfloat16), value, preferred_element_type=jnp.float32
                )
            return 0

        lax.fori_loop(first, stop, block, 0)

    def attend_for_top(i):
        g = group_of(i)
        q_copy(i).wait_recv()
        blocks(
            g, lambda hd: q_top[i, :, hd * HEAD_DIM:(hd + 1) * HEAD_DIM],
            top_doc, top, max(top - steps, 0), top,
        )
        for hd in range(pair):
            o_top[i, :, hd * HEAD_DIM:(hd + 1) * HEAD_DIM] = acc[hd].astype(jnp.bfloat16)
            line = jnp.broadcast_to(tot[hd], (tokens, 128)).T
            t_top[i, hd * 4:(hd + 1) * 4, :] = line[0:4, :]
        o_copy(i).start()
        t_copy(i).start()

    def attend_group(i):
        g = group_of(i)

        def query(hd):
            return q_ref[:, pl.ds(pl.multiple_of((g * pair + hd) * HEAD_DIM, 128), HEAD_DIM)]

        blocks(g, query, own_doc, z, lo, z + 1)

        @pl.when(z == top)
        def _():
            o_copy(i).wait_recv()
            t_copy(i).wait_recv()
            for hd in range(pair):
                part = o_top[i, :, hd * HEAD_DIM:(hd + 1) * HEAD_DIM]
                acc[hd] = acc[hd] + part.astype(jnp.float32)
                line = t_top[i, hd * 4:hd * 4 + 1, :]
                tot[hd] = tot[hd] + jnp.broadcast_to(line, (128, tokens)).T[:, 0:1]

        for hd in range(pair):
            cols = pl.ds(pl.multiple_of((g * pair + hd) * HEAD_DIM, 128), HEAD_DIM)
            att[:, cols] = (acc[hd] / tot[hd]).astype(att.dtype)

    tree = [[0] + list(order) for order in orders(bits)]

    def first_bit(r, h):
        for b in tree[h]:
            if r & (1 << b):
                return b

    def sources(r, h):
        out = []
        for b in tree[h]:
            if r & (1 << b):
                break
            out.append(r | (1 << b))
        return out

    ahead_of = 2

    def block_t(r):
        start = pl.multiple_of(flip(me, r) * big, 128)
        return att[:, pl.ds(start, big)].T

    def reduce_block(r, h, block):
        value = jnp.dot(
            block, cot_ref[:, h * half:(h + 1) * half], preferred_element_type=jnp.float32
        )
        for src in sources(r, h):
            if (r, h) == (0, 1) and src == ahead_of:
                continue
            descriptor(
                sb.at[h, src], rb.at[h, src], bs.at[h], br.at[h, src], me, right
            ).wait_recv()
            value = value + rb[h, src].astype(jnp.float32)
        if r == 0:
            grad[:, h * half:(h + 1) * half] = value
            return
        if (r, h) == (ahead_of, 1):
            extra[...] = value
            return
        sb[h, r] = value.astype(jnp.bfloat16)
        b = first_bit(r, h)
        go(lambda: descriptor(
            sb.at[h, r], rb.at[h, r], bs.at[h], br.at[h, r], flip(me, 1 << b), z
        ), None, False)

    def x_copy():
        return descriptor(x_s, x_r, xs.at[0], xs.at[1], flip(me, ahead_of), z)

    def line_copy(job, direction, k):
        return descriptor(
            zs.at[job, direction, k], zr.at[job, direction, k],
            zss.at[job, direction, k], zsr.at[job, direction, k],
            me, right if direction == 0 else left,
        )

    def rows_of(job, dest):
        at = pl.ds(pl.multiple_of(dest * rows, 16), rows)
        if job == 2:
            return extra[at, :]
        return grad[at, job * half:(job + 1) * half]

    def line_hop(job, direction, k, cond, relay):
        dest = n - 1 - k if direction == 0 else k

        @pl.when(cond)
        def _():
            value = rows_of(job, dest)
            if relay:
                line_copy(job, direction, k).wait_recv()
                value = value + zr[job, direction, k].astype(jnp.float32)
            zs[job, direction, k] = value.astype(jnp.bfloat16)
            line_copy(job, direction, k).start()

        sends.append((lambda: line_copy(job, direction, k), cond))

    def line_push(job):
        for k in range(n - 1):
            line_hop(job, 0, k, z == 0, False)
            line_hop(job, 1, k, z == top, False)

    def line_relay(job, direction, only=True):
        for k in range(n - 2):
            if direction == 0:
                line_hop(job, 0, k, (z > 0) & (z < n - 1 - k) & only, True)
            else:
                line_hop(job, 1, k, (z < top) & (z > k) & only, True)

    def line_final(job):
        target, cols = own_ref, slice(job * half, (job + 1) * half)
        if job == 2:
            target, cols = own_extra, slice(0, half)
        target[:, cols] = rows_of(job, z)
        for direction, cond, k in ((0, z > 0, top - z), (1, z < top, z)):

            @pl.when(cond)
            def _(direction=direction, k=k):
                line_copy(job, direction, k).wait_recv()
                target[:, cols] = target[:, cols] + zr[job, direction, k].astype(jnp.float32)

        if job == 2:
            x_s[...] = own_extra[...].astype(jnp.bfloat16)
            go(x_copy)

    late = []
    for i in range(KV_HEADS):
        if i == KV_HEADS // 2:
            early = len(sends)
        kv_relay(i)
        if hops and i + ahead < KV_HEADS:
            kv_send_next = i + ahead
            go(
                lambda j=kv_send_next: kv_copy(1, j, z), (z > 0) & kv_room(1), False
            )
        for act in events[i]:
            act()
        if i == 0:
            load_cot.wait()
            for make in doc_copies:
                make().wait_recv()
            line = doc_all[0:1, top * tokens:(top + 1) * tokens]
            top_doc[...] = jnp.broadcast_to(line, (128, tokens)).T

        @pl.when(z == top - 1)
        def _():
            attend_for_top(i)

        attend_group(i)
        for r, h in late:
            reduce_block(r, h, block_t(r))
        late = []
        for r in range((KV_HEADS - i) * per - 1, (KV_HEADS - 1 - i) * per - 1, -1):
            if r == 0:
                continue
            block = block_t(r)
            for h in range(2):
                if len(sources(r, h)) > 1 and i < 4:
                    late.append((r, h))
                else:
                    reduce_block(r, h, block)
                if (r, h) == (ahead_of, 1):
                    line_push(2)

    def tail_arrive(s):
        for item in chunks:
            if item["at"][1] == s and not item["here"]:
                item["come"]()
        if s + 1 < n:
            w_send(0, s + 1)
            if s >= 3:
                w_send(1, s + 1)

    if n > 2:
        tail_arrive(2)
    last_block = block_t(0)
    reduce_block(0, 1, last_block)
    line_push(1)
    line_relay(2, 0)
    line_relay(1, 0)
    line_relay(2, 1)
    turn(True)
    line_relay(1, 1, helper)
    if n > 3:
        tail_arrive(3)
    reduce_block(0, 0, last_block)
    line_push(0)
    line_relay(0, 0)
    line_relay(1, 1, z < top - 1)
    line_final(2)
    middle = len(sends) - early
    flush(early)
    line_final(1)
    line_relay(0, 1)
    for s in range(4, n):
        turn()
        tail_arrive(s)
    turn()
    turn()
    line_final(0)

    @pl.when(z == top - 1)
    def _():
        sent(o_top, hs.at[1])
        sent(t_top, hs.at[2])

    @pl.when(z == top)
    def _():
        sent(q_top, hs.at[0])

    for s in range(1, hops + 1):

        @pl.when(kv_room(s))
        def _(s=s):
            sent(kv_all.at[:, :, 0:tokens - skips[s - 1], :], ks.at[s - 1])

    sent(doc_all.at[:, 0:(n - 1) * tokens], ds_.at[0])
    sent(sb.at[0, 1:count], bs.at[0])
    sent(sb.at[1, 0:count - 2], bs.at[1])

    x_copy().wait_recv()
    own_ref[:, half:] = own_ref[:, half:] + x_r[...].astype(jnp.float32)

    own = own_ref[...]
    save_own = pltpu.make_async_copy(own_ref, own_hbm, io_sem.at[2])
    save_own.start()
    total = jnp.broadcast_to(
        jnp.sum(jnp.sum(own * own, axis=1, keepdims=True), axis=0, keepdims=True), (8, 128)
    )
    for k in range(bits - 1):
        turn()

    def project(c, _):
        cols = pl.ds(pl.multiple_of(c * 256, 256), 256)
        out_ref[:, cols] = jnp.dot(
            att[...], w_all[:, cols], preferred_element_type=jnp.float32
        ).astype(out_ref.dtype)
        return 0

    tiles = width // 256
    mid = tiles // 2 * 256

    def save(cut, i):
        return pltpu.make_async_copy(out_ref.at[:, cut], out_hbm.at[:, cut], io_sem.at[i])

    save_left, save_right = save(slice(0, mid), 3), save(slice(mid, width), 4)
    stage = [
        [(r, flip(me, r), z) for r in range(1, count)],
        [(count + s - 1, me, lax.rem(z + s, n)) for s in range(1, n)],
    ]
    for j, peers in enumerate(stage):
        tot_s[j] = total
        for i, dp, seq in peers:
            go(lambda i=i, dp=dp, seq=seq, j=j: descriptor(
                tot_s.at[j], tot_r.at[i], qs.at[j], qr.at[j], dp, seq
            ), None, False)
        if j == 0:
            got = w_all.at[0:n * count // 2 * rows, :]
            descriptor(got, got, ts.at[0], ts.at[1], me, right).wait_recv()
            lax.fori_loop(0, tiles // 2, project, 0)
            save_left.start()
        else:
            lax.fori_loop(tiles // 2, tiles, project, 0)
            save_right.start()
        got = tot_r.at[peers[0][0]:peers[-1][0] + 1]
        descriptor(got, got, qs.at[j], qr.at[j], me, right).wait_recv()
        for i, _, _ in peers:
            total = total + tot_r[i]
        sent(got, qs.at[j])
    sum_ref[...] = total
    sent(w_all.at[0:n * (count - 1) * rows, :], ts.at[0])
    flush(len(sends))
    save_own.wait()
    save_left.wait()
    save_right.wait()


def main_step(q, k, v, docs, cot, w, bits, n):
    tokens = k.shape[0]
    rows, width = w.shape
    half = width // 2
    count = 1 << bits
    skips = reach_skips(tokens, n)
    hops = min(len(skips), n - 2)
    sem = pltpu.SemaphoreType.DMA
    vm = pl.BlockSpec(memory_space=pltpu.VMEM)
    hbm = pl.BlockSpec(memory_space=pl.ANY)
    pair = HEADS // KV_HEADS
    bf16, f32 = jnp.bfloat16, jnp.float32
    return pl.pallas_call(
        functools.partial(main_kernel, bits, n, skips, 2),
        out_shape=(
            jax.ShapeDtypeStruct((tokens, width), bf16),
            jax.ShapeDtypeStruct((rows, width), f32),
            jax.ShapeDtypeStruct((8, 128), f32),
        ),
        in_specs=[hbm, vm, vm, vm, hbm, vm],
        out_specs=(hbm, hbm, vm),
        scratch_shapes=[
            pltpu.VMEM(q.shape, q.dtype),
            pltpu.VMEM(cot.shape, cot.dtype),
            pltpu.VMEM((tokens, width), bf16),
            pltpu.VMEM((rows, width), f32),
            sem((5,)),
            pltpu.VMEM((KV_HEADS, 2, n * tokens, HEAD_DIM), bf16),
            pltpu.VMEM((8, n * tokens), jnp.int32),
            pltpu.VMEM((count * n * rows, width), bf16),
            pltpu.VMEM((tokens, HEADS * HEAD_DIM), bf16),
            pltpu.VMEM((tokens, 128), jnp.int32),
            pltpu.VMEM((tokens, 128), jnp.int32),
            pltpu.VMEM((pair, tokens, HEAD_DIM), f32),
            pltpu.VMEM((pair, tokens, 1), f32),
            pltpu.VMEM((KV_HEADS, tokens, pair * HEAD_DIM), bf16),
            pltpu.VMEM((KV_HEADS, tokens, pair * HEAD_DIM), bf16),
            pltpu.VMEM((KV_HEADS, 8, tokens), f32),
            pltpu.VMEM((2, count, n * rows, half), bf16),
            pltpu.VMEM((2, count, n * rows, half), bf16),
            pltpu.VMEM((3, 2, n - 1, rows, half), bf16),
            pltpu.VMEM((3, 2, n - 1, rows, half), bf16),
            pltpu.VMEM((n * rows, width), f32),
            pltpu.VMEM((n * rows, half), f32),
            pltpu.VMEM((rows, half), f32),
            pltpu.VMEM((rows, half), bf16),
            pltpu.VMEM((rows, half), bf16),
            pltpu.VMEM((2, 8, 128), f32),
            pltpu.VMEM((count + n - 1, 8, 128), f32),
            sem((2, n - 1)), sem((2, n - 1)),
            sem((max(hops, 1),)), sem((max(hops, 1), KV_HEADS)),
            sem((1,)), sem((n - 1,)),
            sem((2,)), sem((n, 2, count // 2)),
            sem((2,)), sem((2, count)),
            sem((3, 2, n - 1)), sem((3, 2, n - 1)),
            sem((2,)), sem((2,)),
            sem((3,)), sem((3, KV_HEADS)),
            sem((2,)),
        ],
        compiler_params=pltpu.CompilerParams(
            collective_id=0, has_side_effects=True, vmem_limit_bytes=60 * 1024 * 1024
        ),
    )(q, k, v, docs, cot, w)


def adam_kernel(
    entries, tile,
    grad_ref, sum_ref, w_ref, m1_ref, s1_ref, m2_ref, s2_ref, layer_ref,
    nw_ref, n1_ref, ns1_ref, n2_ref, ns2_ref, layer_out_ref,
    wide, tall1, tall2, out1, out2, hold, sem,
):
    step = pl.program_id(0)
    take = pltpu.make_async_copy(layer_ref, hold, sem.at[0])
    give = pltpu.make_async_copy(hold, layer_out_ref, sem.at[1])

    @pl.when(step == 0)
    def _():
        take.start()

    @pl.when(step == 1)
    def _():
        take.wait()
        give.start()

    rows = w_ref.shape[0]
    groups = s1_ref.shape[0]
    rms = jnp.sqrt(sum_ref[0:1, :] / entries + 1e-06)
    factor = jnp.minimum(1.0, 1.0 / rms)
    lane = lax.broadcasted_iota(jnp.int32, tall1.shape, 1)

    @pl.when(step == 0)
    def _():
        for tall, ref in ((tall1, s1_ref), (tall2, s2_ref)):
            wide[...] = jnp.zeros_like(wide)
            wide[0:groups, 0:rows] = ref[...]
            tall[...] = wide[...].T

    def decode(coded, tall, g):
        x = coded.astype(jnp.float32)
        scale = jnp.sum(jnp.where(lane == g, tall[...], 0.0), axis=-1, keepdims=True)[0:rows]
        root = scale * jnp.sqrt(jnp.abs(x))
        return jnp.where(x < 0, -root, root)

    def encode(x, out, g):
        scale = jnp.max(jnp.abs(x), axis=-1, keepdims=True) + 1e-06
        out[0:rows] = jnp.where(lane[0:rows] == g, scale, out[0:rows])
        return (x * jnp.abs(x) / (scale * scale)).astype(jnp.bfloat16)

    for j in range(tile // GROUP):
        g = step * (tile // GROUP) + j
        cols = slice(j * GROUP, (j + 1) * GROUP)
        clipped = grad_ref[:, cols] * factor
        first = beta_first * decode(m1_ref[:, cols], tall1, g) + (
            1.0 - beta_first
        ) * clipped
        second = (
            beta_second * decode(m2_ref[:, cols], tall2, g)
            + (1.0 - beta_second) * clipped * clipped
        )
        weight = w_ref[:, cols]
        nw_ref[:, cols] = weight - learn_rate * (
            first / (jnp.sqrt(second) + 1e-08) + decay_rate * weight
        )
        n1_ref[:, cols] = encode(first, out1, g)
        n2_ref[:, cols] = encode(second, out2, g)

    @pl.when(step == pl.num_programs(0) - 1)
    def _():
        ns1_ref[...] = out1[...].T[0:groups, 0:rows]
        ns2_ref[...] = out2[...].T[0:groups, 0:rows]
        give.wait()


def adam(layer, grad, total, weight, m1, s1, m2, s2, entries):
    rows, width = weight.shape
    like = lambda a: jax.ShapeDtypeStruct(a.shape, a.dtype)
    s1, s2 = s1.T, s2.T
    lanes = pl.cdiv(rows, 128) * 128
    deep = pl.cdiv(width // GROUP, 128) * 128
    parts = 3
    tile = width // parts
    cut = pl.BlockSpec((rows, tile), lambda i: (0, i))
    whole = lambda a: pl.BlockSpec(a.shape, lambda i: (0, 0))
    scratch = [pltpu.VMEM((deep, lanes), jnp.float32)]
    scratch += [pltpu.VMEM((lanes, deep), jnp.float32)] * 4
    scratch += [pltpu.VMEM(layer.shape, layer.dtype), pltpu.SemaphoreType.DMA((2,))]
    far = pl.BlockSpec(memory_space=pl.ANY)
    nw, n1, ns1, n2, ns2, layer = pl.pallas_call(
        functools.partial(adam_kernel, entries, tile),
        grid=(parts,),
        out_shape=(like(weight), like(m1), like(s1), like(m2), like(s2), like(layer)),
        in_specs=[cut, whole(total), cut, cut, whole(s1), cut, whole(s2), far],
        out_specs=(cut, cut, whole(s1), cut, whole(s2), far),
        scratch_shapes=scratch,
    )(grad, total, weight, m1, s1, m2, s2, layer)
    return layer, nw, n1, ns1.T, n2, ns2.T


def local(
    bits, n,
    queries, keys, values, segments, cotangent, weight,
    first_moment, first_scale, second_moment, second_scale,
):
    rows, width = weight.shape
    layer_out, grad, total = main_step(
        queries[0], keys[0], values[0],
        segments, cotangent[0], weight, bits, n,
    )
    entries = float((1 << bits) * n * rows * width)
    layer_out, *updated = adam(
        layer_out, grad, total, weight,
        first_moment, first_scale, second_moment, second_scale, entries,
    )
    return (layer_out[None], *updated)


def solution(mesh):
    bits = mesh.shape["dp"].bit_length() - 1
    n = mesh.shape["seq"]
    shard = P(("dp", "seq"), None)
    tok = P("dp", "seq", None)
    return jax.shard_map(
        functools.partial(local, bits, n),
        mesh=mesh,
        in_specs=(tok, tok, tok, P("dp", "seq"), tok, shard, shard, shard, shard, shard),
        out_specs=(tok, shard, shard, shard, shard, shard),
        check_vma=False,
    )
```

```python
import functools

import jax
import jax.numpy as jnp
from jax import lax
from jax.experimental import pallas as pl
from jax.experimental.pallas import tpu as pltpu
from jax.sharding import PartitionSpec as P

HEADS = 16
KV_HEADS = 8
HEAD_DIM = 128
GROUP = 128

score_scale = 144.0 ** (-0.5)
soft_cap = 50.0
beta_first = 0.9
beta_second = 0.95
learn_rate = 0.001
decay_rate = 0.1

MESH = pl.DeviceIdType.MESH


def longest(length):
    return length * 5 // 8


def reach_skips(tokens, n):
    skips = []
    for s in range(1, n):
        skip = max(0, s * tokens - longest(n * tokens)) // 128 * 128
        if skip < tokens:
            skips.append(skip)
    return tuple(skips)


def orders(bits):
    high = list(range(1, bits))
    return (high, high[::-1])


def flip(me, r):
    out = me
    b = 0
    while (1 << b) <= r:
        if r & (1 << b):
            digit = lax.rem(lax.div(me, 1 << b), 2)
            out = out + (1 - 2 * digit) * (1 << b)
        b += 1
    return out


def greet(me, z, bits, n):
    barrier = pltpu.get_barrier_semaphore()
    for r in range(1, 1 << bits):
        pl.semaphore_signal(
            barrier, inc=1, device_id={"dp": flip(me, r), "seq": z}, device_id_type=MESH
        )
    for s in range(1, n):
        pl.semaphore_signal(
            barrier, inc=1, device_id={"dp": me, "seq": lax.rem(z + s, n)}, device_id_type=MESH
        )
    pl.semaphore_wait(barrier, (1 << bits) + n - 2)


def main_kernel(
    bits, n, skips, ahead,
    q_hbm, k_ref, v_ref, doc_ref, cot_hbm, w_ref,
    out_hbm, own_hbm, sum_ref,
    q_ref, cot_ref, out_ref, own_ref, io_sem, kv_all, doc_all, w_all, att, own_doc, top_doc, acc, tot, q_top, o_top, t_top,
    sb, rb, zs, zr, grad, extra, own_extra, x_s, x_r, tot_s, tot_r,
    ws, wr, ks, kr, ds_, dr, ts, tr, bs, br, zss, zsr, qs, qr, hs, hr, xs,
):
    me = lax.axis_index("dp")
    z = lax.axis_index("seq")
    tokens = k_ref.shape[0]
    rows, width = w_ref.shape
    half = width // 2
    big = n * rows
    count = 1 << bits
    per = count // KV_HEADS
    steps = len(skips)
    right, left = lax.rem(z + 1, n), lax.rem(z + n - 1, n)
    group_me = lax.div(me, per)
    sends = []
    load_q = pltpu.make_async_copy(q_hbm, q_ref, io_sem.at[0])
    load_cot = pltpu.make_async_copy(cot_hbm, cot_ref, io_sem.at[1])
    load_q.start()
    load_cot.start()

    def descriptor(src, dst, ssem, rsem, dp, seq):
        return pltpu.make_async_remote_copy(
            src_ref=src, dst_ref=dst, send_sem=ssem, recv_sem=rsem,
            device_id={"dp": dp, "seq": seq}, device_id_type=MESH,
        )

    def go(make, cond=None, keep=True):
        if cond is None:
            make().start()
        else:

            @pl.when(cond)
            def _():
                make().start()

        if keep:
            sends.append((make, cond))

    def sent(ref, sem):
        descriptor(ref, ref, sem, sem, me, right).wait_send()

    def flush(upto):
        now, sends[:] = sends[:upto], sends[upto:]
        while now:
            cond = now[0][1]
            same = 1
            while same < len(now) and now[same][1] is cond:
                same += 1
            batch, now = now[:same], now[same:]

            def act(batch=batch):
                for make, _ in batch:
                    make().wait_send()

            when(cond, act)

    def when(cond, act):
        if cond is None:
            act()
        else:
            pl.when(cond)(act)

    own_rows = pl.ds(pl.multiple_of(z * tokens, 128), tokens)

    def group_of(i):
        return flip(group_me, KV_HEADS - 1 - i)

    def restore_group(g, _):
        cols = pl.ds(pl.multiple_of(g * HEAD_DIM, 128), HEAD_DIM)
        for part, ref in enumerate((k_ref, v_ref)):
            x = ref[:, cols].astype(jnp.float32)
            scale = jnp.max(jnp.abs(x), axis=-1, keepdims=True) + 1e-06
            wide = scale.astype(jnp.bfloat16).astype(jnp.float32)
            coded = (x / wide).astype(jnp.bfloat16).astype(jnp.float32)
            kv_all[g, part, own_rows, :] = (coded * wide).astype(jnp.bfloat16)
        return 0

    for i in range(ahead):
        restore_group(group_of(i), 0)
    doc_all[:, own_rows] = jnp.broadcast_to(doc_ref[...], (8, tokens))
    own_doc[...] = jnp.broadcast_to(doc_ref[0:1, :], (128, tokens)).T

    def w_rows(block, zz):
        return pl.ds(pl.multiple_of((block * n + zz) * rows, 16), rows)

    w_all[w_rows(me, z), :] = w_ref[...].astype(jnp.bfloat16)
    for s in range(1, min(steps, n - 2) + 1):
        if skips[s - 1]:

            @pl.when((z >= s) & (z < n - 1))
            def _(s=s):
                stale = pl.ds(pl.multiple_of((z - s) * tokens, 128), skips[s - 1])
                for g in range(KV_HEADS):
                    for part in range(2):
                        kv_all[g, part, stale, :] = jnp.zeros(
                            (skips[s - 1], HEAD_DIM), jnp.bfloat16
                        )

    greet(me, z, bits, n)

    def room(direction, s):
        if direction == 0:
            return (z >= s - 1) & (z < n - 1)
        return (z <= n - s) & (z > 0)

    def landed(direction, s):
        return z >= s if direction == 0 else z <= n - 1 - s

    hops = min(steps, n - 2)
    top = n - 1

    def kv_room(s):
        return (z >= s - 1) & (z < top - 1)

    def kv_landed(s):
        return (z >= s) & (z < top)

    def kv_copy(s, i, at):
        skip = skips[s - 1]
        start = pl.multiple_of(at * tokens + skip, 128)
        part = kv_all.at[group_of(i), :, pl.ds(start, tokens - skip), :]
        return descriptor(part, part, ks.at[s - 1], kr.at[s - 1, i], me, right)

    def kv_send(s, i, cond):
        go(lambda: kv_copy(s, i, z - (s - 1)), cond, False)

    def kv_relay(i):
        for s in range(1, hops + 1):

            @pl.when(kv_landed(s))
            def _(s=s):
                kv_copy(s, i, z - s).wait_recv()

            if s < hops:
                kv_send(s + 1, i, kv_room(s + 1))

    def w_hop(direction, s, at):
        part = w_all.at[w_rows(me, at), :]
        return descriptor(
            part, part, ws.at[direction, s - 1], wr.at[direction, s - 1],
            me, right if direction == 0 else left,
        )

    def w_send(direction, s, cond=None):
        at = z - (s - 1) if direction == 0 else z + (s - 1)
        cond = room(direction, s) if cond is None else cond
        go(lambda: w_hop(direction, s, at), cond)

    w_tree = [list(order) + [0] for order in orders(bits)]
    w_stage = []
    for h in range(2):
        seen, levels = [0], []
        for b in w_tree[h]:
            fresh = [r | (1 << b) for r in seen]
            levels.append(fresh)
            seen = seen + fresh
        w_stage.append(levels)

    def w_sem(zz, h, r):
        return ts.at[1] if r % 2 else tr.at[zz, h, r // 2]

    def w_forward(zz, h, r, cond):
        order = w_tree[h]
        last = -1
        for i, b in enumerate(order):
            if r & (1 << b):
                last = i
        for b in order[last + 1:]:
            nr = r | (1 << b)

            def make(b=b, nr=nr):
                part = w_all.at[w_rows(flip(me, r), zz), pl.ds(h * half, half)]
                return descriptor(
                    part, part, ts.at[0], w_sem(zz, h, nr), flip(me, 1 << b), z
                )

            go(make, cond, False)

    def w_wait(zz, h, r, cond):
        def act():
            part = w_all.at[w_rows(flip(me, r), zz), pl.ds(h * half, half)]
            descriptor(part, part, ts.at[0], w_sem(zz, h, r), me, right).wait_recv()

        when(cond, act)

    def w_level(zz, level, cond):
        for j in range(len(w_stage[0][level])):
            for h in range(2):
                r = w_stage[h][level][j]
                w_wait(zz, h, r, cond)
                if level < bits - 1:
                    w_forward(zz, h, r, cond)

    def source(direction, s):
        return z - s if direction == 0 else z + s

    def source(direction, s):
        return z - s if direction == 0 else z + s

    def land(direction, s, cond):
        @pl.when(cond)
        def _():
            w_hop(direction, s, source(direction, s)).wait_recv()

    def spread(direction, s, cond):
        for h in range(2):
            w_forward(source(direction, s), h, 0, cond)

    def level(direction, s, k, cond=None):
        if s == 0:
            w_level(z, k, None)
        else:
            cond = landed(direction, s) if cond is None else cond
            w_level(source(direction, s), k, cond)

    events = {i: [] for i in range(KV_HEADS)}

    def plan(i, act):
        events[min(i, KV_HEADS - 1)].append(act)

    chunks = []

    def chunk(direction, s, cond, lands=None, spreads=None, sees=(), soon=False):
        item = {"at": (direction, s, cond), "done": 0, "landed": False, "here": False, "soon": soon}
        chunks.append(item)

        def touch():
            land(direction, s, cond)
            item["landed"] = True

        def come():
            if not item["landed"]:
                touch()
            spread(direction, s, cond)
            item["here"] = True

        def deeper():
            level(direction, s, item["done"], cond)
            item["done"] += 1

        item["come"], item["deeper"] = come, deeper
        if lands is not None:
            plan(lands, touch)
        if spreads is not None:
            plan(spreads, come)
        for i in sees[:bits - 1]:
            plan(i, deeper)

    def turn(soon=False):
        for item in chunks:
            if soon and not item["soon"]:
                continue
            if item["here"] and item["done"] < bits - 1:
                item["deeper"]()

    at_top, helper, below = z == top, z == top - 1, (z > 0) & (z < top - 1)
    for k in range(bits - 1):
        plan(2 * k, lambda k=k: level(0, 0, k))
    chunk(1, 1, landed(1, 1), 1, 1, (5,))
    chunk(0, 1, at_top, None, 0, (0, 1))
    chunk(0, 1, helper & (z > 0), 0, 0, (3,))
    chunk(0, 1, below, None, 7, soon=True)
    if n > 2:
        plan(1, lambda: w_send(1, 2))
        plan(0, lambda: w_send(0, 2, helper & (z > 0)))
        plan(7, lambda: w_send(0, 2, below))
        chunk(0, 2, at_top, None, 0, (2,), soon=True)
        chunk(1, 2, landed(1, 2), 7, 7, soon=True)
        chunk(0, 2, landed(0, 2) & (z < top))
    if n > 3:
        plan(7, lambda: w_send(1, 3))
    for s in range(3, n):
        chunk(0, s, landed(0, s))
        chunk(1, s, landed(1, s))

    pair = HEADS // KV_HEADS
    span = pair * HEAD_DIM

    def q_cols(i):
        return pl.ds(pl.multiple_of(group_of(i) * span, 128), span)

    def q_copy(i):
        return descriptor(
            q_ref.at[:, q_cols(i)], q_top.at[i], hs.at[0], hr.at[0, i], me, left
        )

    def o_copy(i):
        return descriptor(
            o_top.at[i], o_top.at[i], hs.at[1], hr.at[1, i], me, right
        )

    def t_copy(i):
        return descriptor(
            t_top.at[i], t_top.at[i], hs.at[2], hr.at[2, i], me, right
        )

    load_q.wait()
    doc_copies = []
    for s in range(1, n):
        def make(s=s):
            slot = doc_all.at[:, own_rows]
            return descriptor(
                slot, slot, ds_.at[0], dr.at[s - 1], me, lax.rem(z + s, n)
            )

        go(make, None, False)
        doc_copies.append(make)
    for i in range(ahead):
        if hops:
            kv_send(1, i, kv_room(1))
        go(lambda i=i: q_copy(i), z == top, False)
        if i == 0:
            w_send(0, 1, (z > 0) & (z < top))
        if i == 1:
            w_send(1, 1)
            w_send(0, 1, (z == 0) & (z < top))
    for h in range(2):
        w_forward(z, h, 0, None)
    for i in range(ahead, KV_HEADS):
        restore_group(group_of(i), 0)
        if hops:
            kv_send(1, i, (z == 0) & kv_room(1))
        go(lambda i=i: q_copy(i), z == top, False)

    query_at = lax.broadcasted_iota(jnp.int32, (tokens, tokens), 0)
    key_at = lax.broadcasted_iota(jnp.int32, (tokens, tokens), 1)
    lo = jnp.where(z == top, z, jnp.maximum(z - steps, 0))

    def blocks(g, query, docs_ref, at_block, first, stop):
        acc[...] = jnp.zeros_like(acc)
        tot[...] = jnp.zeros_like(tot)

        def block(j, _):
            at = pl.ds(pl.multiple_of(j * tokens, 128), tokens)
            same = docs_ref[:, 0:1] == doc_all[0:1, at]
            allowed = same & (key_at + (j - at_block) * tokens <= query_at)
            key = kv_all[g, 0, at, :]
            value = kv_all[g, 1, at, :]
            for hd in range(pair):
                scores = lax.dot_general(
                    query(hd), key, (((1,), (1,)), ((), ())),
                    preferred_element_type=jnp.float32,
                )
                capped = soft_cap * jnp.tanh(scores * (score_scale / soft_cap))
                weights = jnp.where(allowed, jnp.exp(capped), 0.0)
                tot[hd] = tot[hd] + jnp.sum(weights, axis=-1, keepdims=True)
                acc[hd] = acc[hd] + jnp.dot(
                    weights.astype(jnp.bfloat16), value, preferred_element_type=jnp.float32
                )
            return 0

        lax.fori_loop(first, stop, block, 0)

    def attend_for_top(i):
        g = group_of(i)
        q_copy(i).wait_recv()
        blocks(
            g, lambda hd: q_top[i, :, hd * HEAD_DIM:(hd + 1) * HEAD_DIM],
            top_doc, top, max(top - steps, 0), top,
        )
        for hd in range(pair):
            o_top[i, :, hd * HEAD_DIM:(hd + 1) * HEAD_DIM] = acc[hd].astype(jnp.bfloat16)
            line = jnp.broadcast_to(tot[hd], (tokens, 128)).T
            t_top[i, hd * 4:(hd + 1) * 4, :] = line[0:4, :]
        o_copy(i).start()
        t_copy(i).start()

    def attend_group(i):
        g = group_of(i)

        def query(hd):
            return q_ref[:, pl.ds(pl.multiple_of((g * pair + hd) * HEAD_DIM, 128), HEAD_DIM)]

        blocks(g, query, own_doc, z, lo, z + 1)

        @pl.when(z == top)
        def _():
            o_copy(i).wait_recv()
            t_copy(i).wait_recv()
            for hd in range(pair):
                part = o_top[i, :, hd * HEAD_DIM:(hd + 1) * HEAD_DIM]
                acc[hd] = acc[hd] + part.astype(jnp.float32)
                line = t_top[i, hd * 4:hd * 4 + 1, :]
                tot[hd] = tot[hd] + jnp.broadcast_to(line, (128, tokens)).T[:, 0:1]

        for hd in range(pair):
            cols = pl.ds(pl.multiple_of((g * pair + hd) * HEAD_DIM, 128), HEAD_DIM)
            att[:, cols] = (acc[hd] / tot[hd]).astype(att.dtype)

    tree = [[0] + list(order) for order in orders(bits)]

    def first_bit(r, h):
        for b in tree[h]:
            if r & (1 << b):
                return b

    def sources(r, h):
        out = []
        for b in tree[h]:
            if r & (1 << b):
                break
            out.append(r | (1 << b))
        return out

    ahead_of = 2

    def block_t(r):
        start = pl.multiple_of(flip(me, r) * big, 128)
        return att[:, pl.ds(start, big)].T

    def reduce_block(r, h, block):
        value = jnp.dot(
            block, cot_ref[:, h * half:(h + 1) * half], preferred_element_type=jnp.float32
        )
        for src in sources(r, h):
            if (r, h) == (0, 1) and src == ahead_of:
                continue
            descriptor(
                sb.at[h, src], rb.at[h, src], bs.at[h], br.at[h, src], me, right
            ).wait_recv()
            value = value + rb[h, src].astype(jnp.float32)
        if r == 0:
            grad[:, h * half:(h + 1) * half] = value
            return
        if (r, h) == (ahead_of, 1):
            extra[...] = value
            return
        sb[h, r] = value.astype(jnp.bfloat16)
        b = first_bit(r, h)
        go(lambda: descriptor(
            sb.at[h, r], rb.at[h, r], bs.at[h], br.at[h, r], flip(me, 1 << b), z
        ), None, False)

    def x_copy():
        return descriptor(x_s, x_r, xs.at[0], xs.at[1], flip(me, ahead_of), z)

    def line_copy(job, direction, k):
        return descriptor(
            zs.at[job, direction, k], zr.at[job, direction, k],
            zss.at[job, direction, k], zsr.at[job, direction, k],
            me, right if direction == 0 else left,
        )

    def rows_of(job, dest):
        at = pl.ds(pl.multiple_of(dest * rows, 16), rows)
        if job == 2:
            return extra[at, :]
        return grad[at, job * half:(job + 1) * half]

    def line_hop(job, direction, k, cond, relay):
        dest = n - 1 - k if direction == 0 else k

        @pl.when(cond)
        def _():
            value = rows_of(job, dest)
            if relay:
                line_copy(job, direction, k).wait_recv()
                value = value + zr[job, direction, k].astype(jnp.float32)
            zs[job, direction, k] = value.astype(jnp.bfloat16)
            line_copy(job, direction, k).start()

        sends.append((lambda: line_copy(job, direction, k), cond))

    def line_push(job):
        for k in range(n - 1):
            line_hop(job, 0, k, z == 0, False)
            line_hop(job, 1, k, z == top, False)

    def line_relay(job, direction, only=True):
        for k in range(n - 2):
            if direction == 0:
                line_hop(job, 0, k, (z > 0) & (z < n - 1 - k) & only, True)
            else:
                line_hop(job, 1, k, (z < top) & (z > k) & only, True)

    def line_final(job):
        target, cols = own_ref, slice(job * half, (job + 1) * half)
        if job == 2:
            target, cols = own_extra, slice(0, half)
        target[:, cols] = rows_of(job, z)
        for direction, cond, k in ((0, z > 0, top - z), (1, z < top, z)):

            @pl.when(cond)
            def _(direction=direction, k=k):
                line_copy(job, direction, k).wait_recv()
                target[:, cols] = target[:, cols] + zr[job, direction, k].astype(jnp.float32)

        if job == 2:
            x_s[...] = own_extra[...].astype(jnp.bfloat16)
            go(x_copy)

    late = []
    for i in range(KV_HEADS):
        if i == KV_HEADS // 2:
            early = len(sends)
        kv_relay(i)
        if hops and i + ahead < KV_HEADS:
            kv_send_next = i + ahead
            go(
                lambda j=kv_send_next: kv_copy(1, j, z), (z > 0) & kv_room(1), False
            )
        for act in events[i]:
            act()
        if i == 0:
            load_cot.wait()
            for make in doc_copies:
                make().wait_recv()
            line = doc_all[0:1, top * tokens:(top + 1) * tokens]
            top_doc[...] = jnp.broadcast_to(line, (128, tokens)).T

        @pl.when(z == top - 1)
        def _():
            attend_for_top(i)

        attend_group(i)
        for r, h in late:
            reduce_block(r, h, block_t(r))
        late = []
        for r in range((KV_HEADS - i) * per - 1, (KV_HEADS - 1 - i) * per - 1, -1):
            if r == 0:
                continue
            block = block_t(r)
            for h in range(2):
                if len(sources(r, h)) > 1 and i < 4:
                    late.append((r, h))
                else:
                    reduce_block(r, h, block)
                if (r, h) == (ahead_of, 1):
                    line_push(2)

    def tail_arrive(s):
        for item in chunks:
            if item["at"][1] == s and not item["here"]:
                item["come"]()
        if s + 1 < n:
            w_send(0, s + 1)
            if s >= 3:
                w_send(1, s + 1)

    if n > 2:
        tail_arrive(2)
    last_block = block_t(0)
    reduce_block(0, 1, last_block)
    line_push(1)
    line_relay(2, 0)
    line_relay(2, 1, helper)
    line_relay(1, 0)
    line_relay(2, 1, z < top - 1)
    turn(True)
    line_relay(1, 1, helper)
    if n > 3:
        tail_arrive(3)
    reduce_block(0, 0, last_block)
    line_push(0)
    line_relay(0, 0)
    line_relay(1, 1, z < top - 1)
    line_final(2)
    middle = len(sends) - early
    flush(early)
    line_final(1)
    line_relay(0, 1)
    for s in range(4, n):
        turn()
        tail_arrive(s)
    turn()
    turn()
    line_final(0)

    @pl.when(z == top - 1)
    def _():
        sent(o_top, hs.at[1])
        sent(t_top, hs.at[2])

    @pl.when(z == top)
    def _():
        sent(q_top, hs.at[0])

    for s in range(1, hops + 1):

        @pl.when(kv_room(s))
        def _(s=s):
            sent(kv_all.at[:, :, 0:tokens - skips[s - 1], :], ks.at[s - 1])

    sent(doc_all.at[:, 0:(n - 1) * tokens], ds_.at[0])
    sent(sb.at[0, 1:count], bs.at[0])
    sent(sb.at[1, 0:count - 2], bs.at[1])

    x_copy().wait_recv()
    own_ref[:, half:] = own_ref[:, half:] + x_r[...].astype(jnp.float32)

    own = own_ref[...]
    save_own = pltpu.make_async_copy(own_ref, own_hbm, io_sem.at[2])
    save_own.start()
    total = jnp.broadcast_to(
        jnp.sum(jnp.sum(own * own, axis=1, keepdims=True), axis=0, keepdims=True), (8, 128)
    )
    for k in range(bits - 1):
        turn()

    def project(c, _):
        cols = pl.ds(pl.multiple_of(c * 256, 256), 256)
        out_ref[:, cols] = jnp.dot(
            att[...], w_all[:, cols], preferred_element_type=jnp.float32
        ).astype(out_ref.dtype)
        return 0

    tiles = width // 256
    mid = tiles // 2 * 256

    def save(cut, i):
        return pltpu.make_async_copy(out_ref.at[:, cut], out_hbm.at[:, cut], io_sem.at[i])

    save_left, save_right = save(slice(0, mid), 3), save(slice(mid, width), 4)
    stage = [
        [(r, flip(me, r), z) for r in range(1, count)],
        [(count + s - 1, me, lax.rem(z + s, n)) for s in range(1, n)],
    ]
    for j, peers in enumerate(stage):
        tot_s[j] = total
        for i, dp, seq in peers:
            go(lambda i=i, dp=dp, seq=seq, j=j: descriptor(
                tot_s.at[j], tot_r.at[i], qs.at[j], qr.at[j], dp, seq
            ), None, False)
        if j == 0:
            got = w_all.at[0:n * count // 2 * rows, :]
            descriptor(got, got, ts.at[0], ts.at[1], me, right).wait_recv()
            lax.fori_loop(0, tiles // 2, project, 0)
            save_left.start()
        else:
            lax.fori_loop(tiles // 2, tiles, project, 0)
            save_right.start()
        got = tot_r.at[peers[0][0]:peers[-1][0] + 1]
        descriptor(got, got, qs.at[j], qr.at[j], me, right).wait_recv()
        for i, _, _ in peers:
            total = total + tot_r[i]
        sent(got, qs.at[j])
    sum_ref[...] = total
    sent(w_all.at[0:n * (count - 1) * rows, :], ts.at[0])
    flush(len(sends))
    save_own.wait()
    save_left.wait()
    save_right.wait()


def main_step(q, k, v, docs, cot, w, bits, n):
    tokens = k.shape[0]
    rows, width = w.shape
    half = width // 2
    count = 1 << bits
    skips = reach_skips(tokens, n)
    hops = min(len(skips), n - 2)
    sem = pltpu.SemaphoreType.DMA
    vm = pl.BlockSpec(memory_space=pltpu.VMEM)
    hbm = pl.BlockSpec(memory_space=pl.ANY)
    pair = HEADS // KV_HEADS
    bf16, f32 = jnp.bfloat16, jnp.float32
    return pl.pallas_call(
        functools.partial(main_kernel, bits, n, skips, 2),
        out_shape=(
            jax.ShapeDtypeStruct((tokens, width), bf16),
            jax.ShapeDtypeStruct((rows, width), f32),
            jax.ShapeDtypeStruct((8, 128), f32),
        ),
        in_specs=[hbm, vm, vm, vm, hbm, vm],
        out_specs=(hbm, hbm, vm),
        scratch_shapes=[
            pltpu.VMEM(q.shape, q.dtype),
            pltpu.VMEM(cot.shape, cot.dtype),
            pltpu.VMEM((tokens, width), bf16),
            pltpu.VMEM((rows, width), f32),
            sem((5,)),
            pltpu.VMEM((KV_HEADS, 2, n * tokens, HEAD_DIM), bf16),
            pltpu.VMEM((8, n * tokens), jnp.int32),
            pltpu.VMEM((count * n * rows, width), bf16),
            pltpu.VMEM((tokens, HEADS * HEAD_DIM), bf16),
            pltpu.VMEM((tokens, 128), jnp.int32),
            pltpu.VMEM((tokens, 128), jnp.int32),
            pltpu.VMEM((pair, tokens, HEAD_DIM), f32),
            pltpu.VMEM((pair, tokens, 1), f32),
            pltpu.VMEM((KV_HEADS, tokens, pair * HEAD_DIM), bf16),
            pltpu.VMEM((KV_HEADS, tokens, pair * HEAD_DIM), bf16),
            pltpu.VMEM((KV_HEADS, 8, tokens), f32),
            pltpu.VMEM((2, count, n * rows, half), bf16),
            pltpu.VMEM((2, count, n * rows, half), bf16),
            pltpu.VMEM((3, 2, n - 1, rows, half), bf16),
            pltpu.VMEM((3, 2, n - 1, rows, half), bf16),
            pltpu.VMEM((n * rows, width), f32),
            pltpu.VMEM((n * rows, half), f32),
            pltpu.VMEM((rows, half), f32),
            pltpu.VMEM((rows, half), bf16),
            pltpu.VMEM((rows, half), bf16),
            pltpu.VMEM((2, 8, 128), f32),
            pltpu.VMEM((count + n - 1, 8, 128), f32),
            sem((2, n - 1)), sem((2, n - 1)),
            sem((max(hops, 1),)), sem((max(hops, 1), KV_HEADS)),
            sem((1,)), sem((n - 1,)),
            sem((2,)), sem((n, 2, count // 2)),
            sem((2,)), sem((2, count)),
            sem((3, 2, n - 1)), sem((3, 2, n - 1)),
            sem((2,)), sem((2,)),
            sem((3,)), sem((3, KV_HEADS)),
            sem((2,)),
        ],
        compiler_params=pltpu.CompilerParams(
            collective_id=0, has_side_effects=True, vmem_limit_bytes=60 * 1024 * 1024
        ),
    )(q, k, v, docs, cot, w)


def adam_kernel(
    entries, tile,
    grad_ref, sum_ref, w_ref, m1_ref, s1_ref, m2_ref, s2_ref, layer_ref,
    nw_ref, n1_ref, ns1_ref, n2_ref, ns2_ref, layer_out_ref,
    wide, tall1, tall2, out1, out2, hold, sem,
):
    step = pl.program_id(0)
    take = pltpu.make_async_copy(layer_ref, hold, sem.at[0])
    give = pltpu.make_async_copy(hold, layer_out_ref, sem.at[1])

    @pl.when(step == 0)
    def _():
        take.start()

    @pl.when(step == 1)
    def _():
        take.wait()
        give.start()

    rows = w_ref.shape[0]
    groups = s1_ref.shape[0]
    rms = jnp.sqrt(sum_ref[0:1, :] / entries + 1e-06)
    factor = jnp.minimum(1.0, 1.0 / rms)
    lane = lax.broadcasted_iota(jnp.int32, tall1.shape, 1)

    @pl.when(step == 0)
    def _():
        for tall, ref in ((tall1, s1_ref), (tall2, s2_ref)):
            wide[...] = jnp.zeros_like(wide)
            wide[0:groups, 0:rows] = ref[...]
            tall[...] = wide[...].T

    def decode(coded, tall, g):
        x = coded.astype(jnp.float32)
        scale = jnp.sum(jnp.where(lane == g, tall[...], 0.0), axis=-1, keepdims=True)[0:rows]
        root = scale * jnp.sqrt(jnp.abs(x))
        return jnp.where(x < 0, -root, root)

    def encode(x, out, g):
        scale = jnp.max(jnp.abs(x), axis=-1, keepdims=True) + 1e-06
        out[0:rows] = jnp.where(lane[0:rows] == g, scale, out[0:rows])
        return (x * jnp.abs(x) / (scale * scale)).astype(jnp.bfloat16)

    for j in range(tile // GROUP):
        g = step * (tile // GROUP) + j
        cols = slice(j * GROUP, (j + 1) * GROUP)
        clipped = grad_ref[:, cols] * factor
        first = beta_first * decode(m1_ref[:, cols], tall1, g) + (
            1.0 - beta_first
        ) * clipped
        second = (
            beta_second * decode(m2_ref[:, cols], tall2, g)
            + (1.0 - beta_second) * clipped * clipped
        )
        weight = w_ref[:, cols]
        nw_ref[:, cols] = weight - learn_rate * (
            first / (jnp.sqrt(second) + 1e-08) + decay_rate * weight
        )
        n1_ref[:, cols] = encode(first, out1, g)
        n2_ref[:, cols] = encode(second, out2, g)

    @pl.when(step == pl.num_programs(0) - 1)
    def _():
        ns1_ref[...] = out1[...].T[0:groups, 0:rows]
        ns2_ref[...] = out2[...].T[0:groups, 0:rows]
        give.wait()


def adam(layer, grad, total, weight, m1, s1, m2, s2, entries):
    rows, width = weight.shape
    like = lambda a: jax.ShapeDtypeStruct(a.shape, a.dtype)
    s1, s2 = s1.T, s2.T
    lanes = pl.cdiv(rows, 128) * 128
    deep = pl.cdiv(width // GROUP, 128) * 128
    parts = 3
    tile = width // parts
    cut = pl.BlockSpec((rows, tile), lambda i: (0, i))
    whole = lambda a: pl.BlockSpec(a.shape, lambda i: (0, 0))
    scratch = [pltpu.VMEM((deep, lanes), jnp.float32)]
    scratch += [pltpu.VMEM((lanes, deep), jnp.float32)] * 4
    scratch += [pltpu.VMEM(layer.shape, layer.dtype), pltpu.SemaphoreType.DMA((2,))]
    far = pl.BlockSpec(memory_space=pl.ANY)
    nw, n1, ns1, n2, ns2, layer = pl.pallas_call(
        functools.partial(adam_kernel, entries, tile),
        grid=(parts,),
        out_shape=(like(weight), like(m1), like(s1), like(m2), like(s2), like(layer)),
        in_specs=[cut, whole(total), cut, cut, whole(s1), cut, whole(s2), far],
        out_specs=(cut, cut, whole(s1), cut, whole(s2), far),
        scratch_shapes=scratch,
    )(grad, total, weight, m1, s1, m2, s2, layer)
    return layer, nw, n1, ns1.T, n2, ns2.T


def local(
    bits, n,
    queries, keys, values, segments, cotangent, weight,
    first_moment, first_scale, second_moment, second_scale,
):
    rows, width = weight.shape
    layer_out, grad, total = main_step(
        queries[0], keys[0], values[0],
        segments, cotangent[0], weight, bits, n,
    )
    entries = float((1 << bits) * n * rows * width)
    layer_out, *updated = adam(
        layer_out, grad, total, weight,
        first_moment, first_scale, second_moment, second_scale, entries,
    )
    return (layer_out[None], *updated)


def solution(mesh):
    bits = mesh.shape["dp"].bit_length() - 1
    n = mesh.shape["seq"]
    shard = P(("dp", "seq"), None)
    tok = P("dp", "seq", None)
    return jax.shard_map(
        functools.partial(local, bits, n),
        mesh=mesh,
        in_specs=(tok, tok, tok, P("dp", "seq"), tok, shard, shard, shard, shard, shard),
        out_specs=(tok, shard, shard, shard, shard, shard),
        check_vma=False,
    )
```
